1024 devices in a mesh: row: 32 (over x, y, core), th: 4 (over z_hi), ph: 8 (over z_lo).
Axes of the slice: x: 4, y: 4, z: 32 (z_hi: 4, z_lo: 8; z = z_hi * 8 + z_lo), core: 2. Of those that a mesh axis runs over, the one named last changes fastest.
Arguments:
- cells: float32 [8, 128, 64, 1024], P(None, 'row', 'th', 'ph'), may hold values from -2 to 3, as said below
- faces: float32 [3, 128, 64, 1024], P(None, 'row', 'th', 'ph'), may hold values from -3 to 3
Outputs:
- state: float32 [8, 128, 64, 1024], P(None, 'row', 'th', 'ph')
- faces_new: float32 [3, 128, 64, 1024], P(None, 'row', 'th', 'ph')
The draws below stay inside these ranges and needn't reach their ends.
Inputs may be any that keep to these rules, and one draw needn't show every extreme that they name: `cells`: fields 0 and 4 (density, pressure) lie between 0.2 and 3; fields 1 to 3 between -0.5 and 0.5; fields 5 to 7 between -2 and 2.
All inputs are finite; a program needn't handle non-finite values.
Results may differ from the reference program's by a relative error of at most 0.0003.
Values sent between devices are 32-bit elements; how exact they have to be, the bound alone decides.
A program may use at most 32 MiB of HBM per device.

```python
import math
import jax
import jax.numpy as jnp
from jax import lax

CR = 4
NR = 128
NT = 64
NP = 1024
N_ROW = 32


def draw_cells(key, part):
    keys = jax.random.split(key, 4)
    shape = (NR, NT, NP)
    rough_one = jax.random.uniform(keys[0], shape, jnp.float32)
    rough_two = jax.random.uniform(keys[1], shape, jnp.float32)
    density = 0.3 * jnp.exp(rough_one * math.log(10.0))
    pressure = 0.2 * jnp.exp(rough_two * math.log(10.0))
    velocity = jax.random.uniform(keys[2], (3,) + shape, jnp.float32, -0.5, 0.5)
    magnetic = jnp.clip(0.6 * jax.random.normal(keys[3], (3,) + shape, jnp.float32), -2.0, 2.0)
    return jnp.concatenate([density[None], velocity, pressure[None], magnetic], axis=0).astype(jnp.float32)


def level_of(rng, extent, pieces, low, top_value):
    def one(dim, parts):
        heights = jax.random.uniform(jax.random.fold_in(jax.random.fold_in(rng, 6), dim), (parts,), jnp.float32, low / len(pieces), top_value / len(pieces))
        return jnp.repeat(jnp.exp(heights), extent[dim] // parts).reshape((-1,) + (1,) * (len(extent) - dim - 1))

    gain = one(*pieces[0])
    for cut in pieces[1:]:
        gain = gain * one(*cut)
    return gain


def noise(key, dims, width, bound, shards=(), kind=jnp.bfloat16):
    drawn = width * jax.random.normal(key, dims, jnp.float32)
    if shards:
        drawn = drawn * level_of(key, dims, shards, -0.22, 0.18)
    return jnp.clip(drawn, -bound, bound).astype(kind)


def setup_inputs(seed: int = 0) -> dict:
    key_list = jax.random.split(jax.random.key(seed), 3)
    cells = draw_cells(jax.random.fold_in(key_list[2], 71), 0)
    faces = noise(key_list[1], (3, NR, NT, NP), 0.6, 3.0, ((1, 32), (2, 4), (3, 8)), jnp.float32)
    return {"cells": cells, "faces": faces}


adiabatic = 5.0 / 3.0
step_size = 0.05

def pad_ghosts(cells):
    field_ids = jnp.arange(cells.shape[0])
    flipper = jnp.where((field_ids == 2) | (field_ids == 7), -1.0, 1.0).astype(jnp.float32).reshape(-1, 1, 1, 1)
    padded = jnp.concatenate([cells[:, :, :, -1:], cells, cells[:, :, :, :1]], axis=3)
    padded = jnp.concatenate([padded[:, :, :1] * flipper, padded, padded[:, :, -1:] * flipper], axis=2)
    padded = jnp.concatenate([padded[:, :1], padded, padded[:, -1:]], axis=1)
    return padded

def conserved_flux(padded):
    density = padded[0]
    velocity = padded[1:4]
    pressure = padded[4]
    magnetic = padded[5:8]
    kinetic = 0.5 * density * lax.optimization_barrier(jnp.sum(velocity * velocity, axis=0))
    magnetic_sq = lax.optimization_barrier(jnp.sum(magnetic * magnetic, axis=0))
    energy = pressure / (adiabatic - 1.0) + kinetic + 0.5 * magnetic_sq
    total_press = pressure + 0.5 * magnetic_sq
    alignment = lax.optimization_barrier(jnp.sum(velocity * magnetic, axis=0))
    fast_speed = jnp.sqrt((adiabatic * pressure + magnetic_sq) / density)
    conserved = jnp.stack([density, density * velocity[0], density * velocity[1], density * velocity[2], energy])
    fluxes = []
    speeds = []
    for direction in range(3):
        moving = velocity[direction]
        normal_field = magnetic[direction]
        entries = [density * moving]
        for component in range(3):
            moment = density * velocity[component] * moving - magnetic[component] * normal_field
            if component == direction:
                moment = moment + total_press
            entries.append(moment)
        entries.append((energy + total_press) * moving - normal_field * alignment)
        fluxes.append(jnp.stack(entries))
        speeds.append(jnp.abs(moving) + fast_speed)
    return (conserved, fluxes, speeds)

def hydro_change(padded):
    conserved, fluxes, speeds = conserved_flux(padded)
    change = jnp.zeros_like(conserved[:, 1:-1, 1:-1, 1:-1])
    for direction in range(3):
        keeper = [slice(None), slice(1, -1), slice(1, -1), slice(1, -1)]
        keeper[direction + 1] = slice(None)
        lower_cut = [slice(None)] * 4
        upper_cut = [slice(None)] * 4
        lower_cut[direction + 1] = slice(0, -1)
        upper_cut[direction + 1] = slice(1, None)
        state_cut = conserved[tuple(keeper)]
        flux_cut = fluxes[direction][tuple(keeper)]
        speed_cut = speeds[direction][tuple(keeper[1:])]
        wave_speed = jnp.maximum(speed_cut[tuple(lower_cut[1:])], speed_cut[tuple(upper_cut[1:])])
        face_flux = 0.5 * (flux_cut[tuple(lower_cut)] + flux_cut[tuple(upper_cut)]) - 0.5 * wave_speed * (state_cut[tuple(upper_cut)] - state_cut[tuple(lower_cut)])
        change = change + face_flux[tuple(upper_cut)] - face_flux[tuple(lower_cut)]
    return conserved[:, 1:-1, 1:-1, 1:-1] - step_size * change

def edge_fields(padded):
    velocity = padded[1:4]
    magnetic = padded[5:8]
    emf_first = -(velocity[1] * magnetic[2] - velocity[2] * magnetic[1])
    emf_second = -(velocity[2] * magnetic[0] - velocity[0] * magnetic[2])
    emf_third = -(velocity[0] * magnetic[1] - velocity[1] * magnetic[0])
    inner = emf_first[1:-1]
    edge_one = 0.25 * (inner[:, :-1, :-1] + inner[:, 1:, :-1] + inner[:, :-1, 1:] + inner[:, 1:, 1:])
    inner = emf_second[:, 1:-1, :]
    edge_two = 0.25 * (inner[:-1, :, :-1] + inner[1:, :, :-1] + inner[:-1, :, 1:] + inner[1:, :, 1:])
    inner = emf_third[:, :, 1:-1]
    edge_three = 0.25 * (inner[:-1, :-1] + inner[1:, :-1] + inner[:-1, 1:] + inner[1:, 1:])
    return (edge_one, edge_two, edge_three)

def face_advance(first, second, third, edge_one, edge_two, edge_three):
    new_first = first - step_size * (edge_three[:, 1:] - edge_three[:, :-1] - (edge_two[:, :, 1:] - edge_two[:, :, :-1]))
    new_second = second - step_size * (edge_one[:, :, 1:] - edge_one[:, :, :-1] - (edge_three[1:] - edge_three[:-1]))
    new_third = third - step_size * (edge_two[1:] - edge_two[:-1] - (edge_one[:, 1:] - edge_one[:, :-1]))
    return (new_first, new_second, new_third)

def reference(cells, faces):
    padded = pad_ghosts(cells)
    first_ext = jnp.concatenate([faces[0], faces[0][-1:]], axis=0)
    second_ext = jnp.concatenate([faces[1], faces[1][:, -1:]], axis=1)
    third_ext = jnp.concatenate([faces[2], faces[2][:, :, :1]], axis=2)

    def slab(index):
        start = (index * CR).astype(jnp.int32)
        block = lax.dynamic_slice_in_dim(padded, start, CR + 2, 1)
        conserved_new = hydro_change(block)
        edge_one, edge_two, edge_three = edge_fields(block)
        first = lax.dynamic_slice_in_dim(first_ext, start, CR + 1, 0)
        second = lax.dynamic_slice_in_dim(second_ext, start, CR, 0)
        third = lax.dynamic_slice_in_dim(third_ext, start, CR, 0)
        new_first, new_second, new_third = face_advance(first, second, third, edge_one, edge_two, edge_three)
        return (conserved_new, new_first[:CR], new_second[:, :NT], new_third[:, :, :NP])
    outputs = lax.map(slab, jnp.arange(N_ROW, dtype=jnp.int32))
    conserved_new = jnp.moveaxis(outputs[0], 0, 1).reshape(5, NR, NT, NP)
    new_first = outputs[1].reshape(NR, NT, NP)
    new_second = outputs[2].reshape(NR, NT, NP)
    new_third = outputs[3].reshape(NR, NT, NP)
    upper_first = jnp.concatenate([new_first[1:], new_first[-1:]], axis=0)
    upper_second = jnp.concatenate([new_second[:, 1:], jnp.zeros((NR, 1, NP), jnp.float32)], axis=1)
    upper_third = jnp.concatenate([new_third[:, :, 1:], new_third[:, :, :1]], axis=2)
    centred = 0.5 * jnp.stack([new_first + upper_first, new_second + upper_second, new_third + upper_third])
    state = jnp.concatenate([conserved_new, centred], axis=0)
    return (state, jnp.stack([new_first, new_second, new_third]))
```

```python
import jax
import jax.numpy as jnp
from jax import lax
from jax.experimental import pallas as pl
from jax.experimental.pallas import tpu as pltpu
from jax.sharding import PartitionSpec as P

MESH = pl.DeviceIdType.MESH
STEP = 0.05
QUARTER = 0.0125
GAMMA = 5.0 / 3.0

ROW_UP, ROW_DOWN, FACE_R, PACK_UP, PACK_DOWN, TH_UP, TH_DOWN, FACE_T = range(8)
CORNER_UP, CORNER_DOWN, PAIR_UP, PAIR_DOWN, LOW_UP, LOW_DOWN, HIGH_UP, HIGH_DOWN = range(8, 16)
DIRECT = 16


def cell_state(w):
    density, v0, v1, v2, pressure, b0, b1, b2 = w
    kinetic = 0.5 * density * (v0 * v0 + v1 * v1 + v2 * v2)
    magnetic_sq = b0 * b0 + b1 * b1 + b2 * b2
    energy = pressure / (GAMMA - 1.0) + kinetic + 0.5 * magnetic_sq
    conserved = [density, density * v0, density * v1, density * v2, energy]
    return conserved, magnetic_sq


def flux(w, conserved, magnetic_sq, direction):
    density, v0, v1, v2, pressure, b0, b1, b2 = w
    velocity = (v0, v1, v2)
    magnetic = (b0, b1, b2)
    moving = velocity[direction]
    normal = magnetic[direction]
    total_press = pressure + 0.5 * magnetic_sq
    alignment = v0 * b0 + v1 * b1 + v2 * b2
    fast = jnp.sqrt((GAMMA * pressure + magnetic_sq) / density)
    out = [conserved[direction + 1]]
    for component in range(3):
        moment = conserved[component + 1] * moving - magnetic[component] * normal
        if component == direction:
            moment = moment + total_press
        out.append(moment)
    out.append((conserved[4] + total_press) * moving - normal * alignment)
    return out, jnp.abs(moving) + fast


def quantities(w, direction):
    conserved, magnetic_sq = cell_state(w)
    fluxes, speed = flux(w, conserved, magnetic_sq, direction)
    return conserved, fluxes, speed


def face_flux(lower, upper):
    u_low, f_low, s_low = lower
    u_up, f_up, s_up = upper
    half = 0.5 * jnp.maximum(s_low, s_up)
    return [0.5 * (f_low[i] + f_up[i]) - half * (u_up[i] - u_low[i]) for i in range(5)]


def emf(w, component):
    a, b = ((2, 3), (3, 1), (1, 2))[component]
    return -(w[a] * w[b + 4] - w[b] * w[a + 4])


def kernel(
    cells_hbm, faces_hbm, state, faces_new,
    cv, fv, rlo, rhi, f0hi, packs, gp, th_src, gt, f1_src, f1hi, cr_src, cr, pr, e1_own, e1_src, e1f,
    load_sem, send_sem, recv_sem, sem_two, sem_four,
):
    row = lax.axis_index("row")
    th = lax.axis_index("th")
    ph = lax.axis_index("ph")
    rows, ths, phs = lax.axis_size("row"), lax.axis_size("th"), lax.axis_size("ph")
    z = th * phs + ph
    depth = ths * phs
    at_bottom, at_top = row == 0, row == rows - 1
    at_north, at_south = th == 0, th == ths - 1
    first_z = z == 0
    far_sender = (z == phs - 1) | (z == phs) | (z == phs + 1) | (z == 2 * phs - 1)

    def at_z(place):
        return {"row": row, "th": place // phs, "ph": lax.rem(place, phs)}

    def place(dr=0, dt=0, dp=0):
        return {"row": row + dr, "th": th + dt, "ph": lax.rem(ph + dp + phs, phs)}

    barrier = pltpu.get_barrier_semaphore()

    def tell(semaphore, condition, target):
        @pl.when(condition)
        def _():
            pl.semaphore_signal(semaphore, inc=1, device_id=target, device_id_type=MESH)

    for far in (phs - 1, phs, phs + 1, 2 * phs - 1):
        tell(barrier, first_z, {"row": row, "th": far // phs, "ph": far % phs})
    tell(barrier, row < rows - 1, place(dr=1))
    tell(barrier, row > 0, place(dr=-1))
    for hop in (1, 2):
        tell(barrier, z + hop < depth, at_z(z + hop))
        tell(barrier, z - hop >= 0, at_z(z - hop))

    load_cells = pltpu.make_async_copy(cells_hbm, cv, load_sem.at[0])
    load_faces = pltpu.make_async_copy(faces_hbm, fv, load_sem.at[1])
    load_cells.start()
    load_faces.start()

    def copy(kind, src, dst, target, recv=None):
        return pltpu.make_async_remote_copy(
            src_ref=src, dst_ref=dst, send_sem=send_sem.at[kind],
            recv_sem=recv_sem.at[kind if recv is None else recv],
            device_id=target, device_id_type=MESH,
        )

    up_r, down_r = place(dr=1), place(dr=-1)
    up_t, down_t = place(dt=1), place(dt=-1)
    up_p, down_p = place(dp=1), place(dp=-1)
    origin = {"row": row, "th": th * 0, "ph": ph * 0}
    copies = {
        ROW_UP: copy(ROW_UP, cv.at[:, 3], rlo, up_r),
        ROW_DOWN: copy(ROW_DOWN, cv.at[:, 0], rhi, down_r),
        FACE_R: copy(FACE_R, fv.at[0, 0], f0hi, down_r),
        PACK_UP: copy(PACK_UP, packs.at[1], gp.at[0], up_p),
        PACK_DOWN: copy(PACK_DOWN, packs.at[0], gp.at[1], down_p),
        TH_UP: copy(TH_UP, th_src.at[1], gt.at[0], up_t),
        TH_DOWN: copy(TH_DOWN, th_src.at[0], gt.at[1], down_t),
        FACE_T: copy(FACE_T, f1_src, f1hi, down_t),
        CORNER_UP: copy(CORNER_UP, cr_src.at[1], cr.at[0], up_t),
        CORNER_DOWN: copy(CORNER_DOWN, cr_src.at[0], cr.at[1], down_t),
        PAIR_UP: copy(PAIR_UP, gp, pr.at[0], up_r),
        PAIR_DOWN: copy(PAIR_DOWN, gp, pr.at[1], down_r),
        LOW_UP: copy(LOW_UP, e1_src.at[0], e1f.at[0, 0], up_p),
        LOW_DOWN: copy(LOW_DOWN, e1_src.at[0], e1f.at[1, 0], down_p),
        HIGH_UP: copy(HIGH_UP, e1_src.at[1], e1f.at[0, 1], up_p),
        HIGH_DOWN: copy(HIGH_DOWN, e1_src.at[1], e1f.at[1, 1], down_p),
    }
    direct_left = copy(DIRECT, e1_own, e1f.at[0, 1], origin, HIGH_UP)
    direct_right = copy(DIRECT, e1_own, e1f.at[1, 1], origin, HIGH_DOWN)

    def send(kind, condition=None):
        if condition is None:
            copies[kind].start()
        else:
            pl.when(condition)(copies[kind].start)

    def arrived(kind, condition=None):
        if condition is None:
            copies[kind].wait_recv()
        else:
            pl.when(condition)(copies[kind].wait_recv)

    load_cells.wait()
    for r in range(4):
        w = [cv[f, r, 0:1] for f in range(8)]
        e1_own[r : r + 1] = emf(w, 0)
        for f in range(8):
            th_src[0, f * 4 + r : f * 4 + r + 1] = w[f]
            th_src[1, f * 4 + r : f * 4 + r + 1] = cv[f, r, 15:16]
    load_faces.wait()
    for r in range(4):
        f1_src[r : r + 1] = fv[1, r, 0:1]
    for c in range(4):
        turned = cv[2 * c : 2 * c + 2].reshape(128, 128).T
        packs[0, c : c + 1] = turned[0:1]
        packs[1, c : c + 1] = turned[127:128]
    third = fv[2].reshape(64, 128)
    turned = jnp.concatenate([third, third], axis=0).T
    for c in range(4, 8):
        packs[0, c : c + 1] = turned[0:1]
        packs[1, c : c + 1] = turned[127:128]

    @pl.when(at_bottom)
    def _():
        rlo[...] = cv[:, 0]

    @pl.when(at_top)
    def _():
        rhi[...] = cv[:, 3]
        f0hi[...] = fv[0, 3]

    def fill_polar(side, condition):
        @pl.when(condition)
        def _():
            for f in range(8):
                rows_f = th_src[side, f * 4 : f * 4 + 4]
                gt[side, f * 4 : f * 4 + 4] = -rows_f if f in (2, 7) else rows_f

    fill_polar(0, at_north)
    fill_polar(1, at_south)

    def ghost_rows(side):
        return [gt[side, f * 4 : f * 4 + 4] for f in range(8)]

    @pl.when(at_north)
    def _():
        e1_src[0] = emf(ghost_rows(0), 0)

    count = (
        (z >= 1).astype(jnp.int32) + (z >= 2).astype(jnp.int32)
        + (z < depth - 1).astype(jnp.int32) + (z < depth - 2).astype(jnp.int32)
        + (row > 0).astype(jnp.int32) + (row < rows - 1).astype(jnp.int32)
        + far_sender.astype(jnp.int32)
    )
    pl.semaphore_wait(barrier, count)

    pl.when(z == 2 * phs - 1)(direct_left.start)
    pl.when(z == phs + 1)(direct_right.start)
    tell(sem_two, z + 2 < depth, at_z(z + 2))
    tell(sem_two, z - 2 >= 0, at_z(z - 2))
    early_down = z == phs
    send(TH_DOWN, early_down)
    send(FACE_T, early_down)
    near_up = (ph < phs - 1) | (z == phs - 1)
    near_down = ph > 0
    send(PACK_UP, near_up)
    send(PACK_DOWN, near_down)
    send(LOW_UP, at_north & near_up)
    send(LOW_DOWN, at_north & near_down)
    send(ROW_UP, row < rows - 1)
    send(ROW_DOWN, row > 0)
    send(FACE_R, row > 0)

    two = (z >= 2).astype(jnp.int32) + (z < depth - 2).astype(jnp.int32)
    pl.semaphore_wait(sem_two, two)
    tell(sem_four, z + 4 < depth, at_z(z + 4))
    tell(sem_four, z - 4 >= 0, at_z(z - 4))

    arrived(ROW_UP, row > 0)
    arrived(ROW_DOWN, row < rows - 1)
    arrived(FACE_R, row < rows - 1)
    for side, line in ((0, 0), (1, 15)):
        for k, ghost in enumerate((rlo, rhi)):
            w = [ghost[f, line : line + 1] for f in range(8)]
            cr_src[side, k : k + 1] = emf(w, 2)

    def fill_corner(side, line, condition):
        @pl.when(condition)
        def _():
            for k, ghost in enumerate((rlo, rhi)):
                w = [ghost[f, line : line + 1] for f in range(8)]
                w[2] = -w[2]
                cr[side, k : k + 1] = emf(w, 2)

    fill_corner(0, 0, at_north)
    fill_corner(1, 15, at_south)
    send(CORNER_DOWN, early_down)

    four = (z >= 4).astype(jnp.int32) + (z < depth - 4).astype(jnp.int32)
    pl.semaphore_wait(sem_four, four)

    later_down = (th > 0) & jnp.logical_not(early_down)
    send(TH_UP, th < ths - 1)
    send(TH_DOWN, later_down)
    send(FACE_T, later_down)
    send(PACK_UP, jnp.logical_not(near_up))
    send(PACK_DOWN, jnp.logical_not(near_down))
    send(LOW_DOWN, at_north & jnp.logical_not(near_down))
    send(CORNER_UP, th < ths - 1)
    send(CORNER_DOWN, later_down)

    shape = (4, 16, 128)
    lane = lax.broadcasted_iota(jnp.int32, shape, 2)
    line = lax.broadcasted_iota(jnp.int32, shape, 1)
    own = [cv[f] for f in range(8)]

    def ahead_t(x):
        return pltpu.roll(x, 15, 1)

    def behind_t(x):
        return pltpu.roll(x, 1, 1)

    def ahead_p(x):
        return pltpu.roll(x, 127, 2)

    def behind_p(x):
        return pltpu.roll(x, 1, 2)

    low = quantities([rlo[f][None] for f in range(8)], 0)
    mid = quantities(own, 0)
    high = quantities([rhi[f][None] for f in range(8)], 0)

    def tall(a, b, c):
        return jnp.concatenate([a, b, c], axis=0)

    u6 = [tall(low[0][i], mid[0][i], high[0][i]) for i in range(5)]
    g6 = [tall(low[1][i], mid[1][i], high[1][i]) for i in range(5)]
    s6 = tall(low[2], mid[2], high[2])
    face = face_flux(([u[:-1] for u in u6], [g[:-1] for g in g6], s6[:-1]), ([u[1:] for u in u6], [g[1:] for g in g6], s6[1:]))
    for i in range(5):
        state[i] = mid[0][i] - STEP * (face[i][1:] - face[i][:-1])

    arrived(PACK_DOWN)
    arrived(PACK_UP)
    send(PAIR_UP, row < rows - 1)
    send(PAIR_DOWN, row > 0)
    columns = jnp.concatenate([gp[0], gp[1]], axis=0).T

    def column(side, c, half):
        col = columns[half * 64 : half * 64 + 64, side * 8 + c : side * 8 + c + 1]
        return jnp.broadcast_to(col, (64, 128)).reshape(shape)

    left, right = lane == 0, lane == 127
    beside = [
        jnp.where(left, column(0, f // 2, f % 2), jnp.where(right, column(1, f // 2, f % 2), own[f]))
        for f in range(8)
    ]
    upper_third = column(1, 4, 0)
    e1_beside, e2_beside = emf(beside, 0), emf(beside, 1)

    def apply(direction, outer, ahead, behind, is_low, is_high):
        mine = quantities(own, direction)
        edge = quantities(outer, direction)

        def shifted(a, b):
            return jnp.where(is_high, b, ahead(a))

        above = (
            [shifted(mine[0][i], edge[0][i]) for i in range(5)],
            [shifted(mine[1][i], edge[1][i]) for i in range(5)],
            shifted(mine[2], edge[2]),
        )
        upper = face_flux(mine, above)
        lower = face_flux(edge, mine)
        for i in range(5):
            below = jnp.where(is_low, lower[i], behind(upper[i]))
            state[i] = state[i] - STEP * (upper[i] - below)

    apply(2, beside, ahead_p, behind_p, left, right)

    arrived(TH_UP, th > 0)

    @pl.when(th > 0)
    def _():
        e1_src[0] = emf(ghost_rows(0), 0)

    send(LOW_UP, th > 0)
    send(LOW_DOWN, th > 0)
    arrived(TH_DOWN, th < ths - 1)
    arrived(FACE_T, th < ths - 1)
    e1_src[1] = emf(ghost_rows(1), 0)
    send(HIGH_UP, z != phs - 1)
    send(HIGH_DOWN, z != 1)

    north, south = line == 0, line == 15

    def spread(ref, *index):
        return jnp.concatenate([jnp.broadcast_to(ref[index + (slice(start, start + 1),)], (16, 128))[None] for start in spread.rows], axis=0)

    def polar(f):
        spread.rows = [f * 4 + r for r in range(4)]
        return jnp.where(north, spread(gt, 0), jnp.where(south, spread(gt, 1), own[f]))

    outside = [polar(f) for f in range(8)]
    apply(1, outside, ahead_t, behind_t, north, south)
    e1_outside, e3_outside = emf(outside, 0), emf(outside, 2)

    arrived(CORNER_UP, th > 0)
    arrived(CORNER_DOWN, th < ths - 1)
    arrived(PAIR_UP, row > 0)
    arrived(PAIR_DOWN, row < rows - 1)

    def pair_emf(ref, *index):
        rows8 = ref[index] if index else ref[...]
        return -(rows8[1:2] * rows8[2:3] - rows8[0:1] * rows8[3:4])

    pair_rows = [pair_emf(gp, 0), pair_emf(gp, 1), pair_emf(pr, 0, 0), pair_emf(pr, 0, 1), pair_emf(pr, 1, 0), pair_emf(pr, 1, 1)]
    pair_columns = jnp.concatenate(pair_rows + [pair_rows[0], pair_rows[0]], axis=0).T

    def pair_ghost(side):
        lanes = lane[:1]
        parts = []
        for k in range(2):
            near = pair_columns[64:80, k : k + 1] if side == 0 else pair_columns[112:128, k : k + 1]
            far_col = pair_columns[112:128, 2 + k : 3 + k] if side == 0 else pair_columns[64:80, 4 + k : 5 + k]
            edge = at_bottom if side == 0 else at_top
            parts.append(jnp.broadcast_to(jnp.where(edge, near, far_col), (16, 128))[None])
        return jnp.where(lanes == 0, parts[0], parts[1])

    def corner_ghost(k):
        a = jnp.broadcast_to(cr[0, k : k + 1], (16, 128))[None]
        b = jnp.broadcast_to(cr[1, k : k + 1], (16, 128))[None]
        return jnp.where(line[:1] == 0, a, b)

    low_w = [rlo[f][None] for f in range(8)]
    high_w = [rhi[f][None] for f in range(8)]
    e1 = emf(own, 0)
    e2 = tall(emf(low_w, 1), emf(own, 1), emf(high_w, 1))
    e3 = tall(emf(low_w, 2), emf(own, 2), emf(high_w, 2))
    e2_side = tall(pair_ghost(0), e2_beside, pair_ghost(1))
    e3_side = tall(corner_ghost(0), e3_outside, corner_ghost(1))

    six = (6, 16, 128)
    lane6 = lax.broadcasted_iota(jnp.int32, six, 2)
    line6 = lax.broadcasted_iota(jnp.int32, six, 1)
    across_t = jnp.where(line6 == 15, e3_side, ahead_t(e3)) - jnp.where(line6 == 0, e3_side, behind_t(e3))
    across_p = jnp.where(lane6 == 127, e2_side, ahead_p(e2)) - jnp.where(lane6 == 0, e2_side, behind_p(e2))
    curl = across_t - across_p
    new_first = fv[0] - QUARTER * (curl[:4] + curl[1:5])
    new_last = f0hi[...] - QUARTER * (curl[4] + curl[5])
    faces_new[0] = new_first
    last = jnp.where(at_top, new_first[3], new_last)
    state[5] = 0.5 * (new_first + jnp.concatenate([new_first[1:], last[None]], axis=0))

    zero = jnp.zeros(shape, jnp.float32)
    curl = (e2[2:] - e2[:-2]) - (
        jnp.where(south, e1_outside, ahead_t(e1)) - jnp.where(north, e1_outside, behind_t(e1))
    )
    curl_beside = (e2_side[2:] - e2_side[:-2]) - (
        jnp.where(south, zero, ahead_t(e1_beside)) - jnp.where(north, zero, behind_t(e1_beside))
    )
    new_third = fv[2] - QUARTER * (curl + jnp.where(left, curl_beside, behind_p(curl)))
    new_upper = upper_third - QUARTER * (curl + curl_beside)
    faces_new[2] = new_third
    state[7] = 0.5 * (new_third + jnp.where(right, new_upper, ahead_p(new_third)))

    curl = (
        jnp.where(right, e1_beside, ahead_p(e1)) - jnp.where(left, e1_beside, behind_p(e1))
    ) - (e3[2:] - e3[:-2])
    curl_outside = (
        jnp.where(right, zero, ahead_p(e1_outside)) - jnp.where(left, zero, behind_p(e1_outside))
    ) - (e3_side[2:] - e3_side[:-2])
    new_second = fv[1] - QUARTER * (curl + jnp.where(north, curl_outside, behind_t(curl)))
    spread.rows = [0, 1, 2, 3]
    new_upper = spread(f1hi) - QUARTER * (curl + curl_outside)
    new_upper = jnp.where(at_south, 0.0, new_upper)
    faces_new[1] = new_second
    state[6] = 0.5 * (new_second + jnp.where(south, new_upper, ahead_t(new_second)))

    arrived(LOW_UP)
    arrived(LOW_DOWN)
    arrived(HIGH_DOWN)
    arrived(HIGH_UP)
    lane4 = lax.broadcasted_iota(jnp.int32, (4, 128), 1)

    def corner_rows(k):
        a = jnp.where(lane4 == 0, pltpu.roll(e1f[0, k], 1, 1), 0.0)
        b = jnp.where(lane4 == 127, pltpu.roll(e1f[1, k], 127, 1), 0.0)
        return QUARTER * a, QUARTER * b

    a_low, b_low = corner_rows(0)
    a_high, b_high = corner_rows(1)
    keep = jnp.where(at_south, 0.0, 0.5)
    for r in range(4):
        a, b = a_low[r : r + 1], b_low[r : r + 1]
        faces_new[1, r, 0:1] = faces_new[1, r, 0:1] - (b - a)
        state[6, r, 0:1] = state[6, r, 0:1] - 0.5 * (b - a)
        faces_new[2, r, 0:1] = faces_new[2, r, 0:1] - a
        state[7, r, 0:1] = state[7, r, 0:1] - 0.5 * (a + b)
        a, b = a_high[r : r + 1], b_high[r : r + 1]
        state[6, r, 15:16] = state[6, r, 15:16] - keep * (b - a)
        faces_new[2, r, 15:16] = faces_new[2, r, 15:16] + a
        state[7, r, 15:16] = state[7, r, 15:16] + 0.5 * (a + b)

    for kind, condition in (
        (ROW_UP, row < rows - 1), (ROW_DOWN, row > 0), (FACE_R, row > 0), (PACK_UP, None), (PACK_DOWN, None),
        (TH_UP, th < ths - 1), (TH_DOWN, th > 0), (FACE_T, th > 0), (CORNER_UP, th < ths - 1), (CORNER_DOWN, th > 0),
        (PAIR_UP, row < rows - 1), (PAIR_DOWN, row > 0), (LOW_UP, None), (LOW_DOWN, None),
        (HIGH_UP, z != phs - 1), (HIGH_DOWN, z != 1),
    ):
        if condition is None:
            copies[kind].wait_send()
        else:
            pl.when(condition)(copies[kind].wait_send)
    pl.when(z == 2 * phs - 1)(direct_left.wait_send)
    pl.when(z == phs + 1)(direct_right.wait_send)


def on_device(cells, faces):
    f32 = jnp.float32
    return pl.pallas_call(
        kernel,
        out_shape=(jax.ShapeDtypeStruct((8, 4, 16, 128), f32), jax.ShapeDtypeStruct((3, 4, 16, 128), f32)),
        in_specs=[pl.BlockSpec(memory_space=pl.ANY)] * 2,
        out_specs=(pl.BlockSpec(memory_space=pltpu.VMEM),) * 2,
        scratch_shapes=[
            pltpu.VMEM((8, 4, 16, 128), f32),
            pltpu.VMEM((3, 4, 16, 128), f32),
            pltpu.VMEM((8, 16, 128), f32),
            pltpu.VMEM((8, 16, 128), f32),
            pltpu.VMEM((16, 128), f32),
            pltpu.VMEM((2, 8, 128), f32),
            pltpu.VMEM((2, 8, 128), f32),
            pltpu.VMEM((2, 32, 128), f32),
            pltpu.VMEM((2, 32, 128), f32),
            pltpu.VMEM((4, 128), f32),
            pltpu.VMEM((4, 128), f32),
            pltpu.VMEM((2, 2, 128), f32),
            pltpu.VMEM((2, 2, 128), f32),
            pltpu.VMEM((2, 2, 8, 128), f32),
            pltpu.VMEM((4, 128), f32),
            pltpu.VMEM((2, 4, 128), f32),
            pltpu.VMEM((2, 2, 4, 128), f32),
            pltpu.SemaphoreType.DMA((2,)),
            pltpu.SemaphoreType.DMA((17,)),
            pltpu.SemaphoreType.DMA((17,)),
            pltpu.SemaphoreType.REGULAR,
            pltpu.SemaphoreType.REGULAR,
        ],
        name="section",
        compiler_params=pltpu.CompilerParams(collective_id=0, has_side_effects=True),
    )(cells, faces)


def solution(mesh):
    spec = P(None, "row", "th", "ph")
    return jax.shard_map(on_device, mesh=mesh, in_specs=(spec, spec), out_specs=(spec, spec), check_vma=False)
```

```python
import jax
import jax.numpy as jnp
from jax import lax
from jax.experimental import pallas as pl
from jax.experimental.pallas import tpu as pltpu
from jax.sharding import PartitionSpec as P

MESH = pl.DeviceIdType.MESH
STEP = 0.05
QUARTER = 0.0125
GAMMA = 5.0 / 3.0

ROW_UP, ROW_DOWN, FACE_R, PACK_UP, PACK_DOWN, TH_UP, TH_DOWN, FACE_T = range(8)
CORNER_UP, CORNER_DOWN, PAIR_UP, PAIR_DOWN, LOW_UP, LOW_DOWN, HIGH_UP, HIGH_DOWN = range(8, 16)
DIRECT = 16


def cell_state(w):
    density, v0, v1, v2, pressure, b0, b1, b2 = w
    kinetic = 0.5 * density * (v0 * v0 + v1 * v1 + v2 * v2)
    magnetic_sq = b0 * b0 + b1 * b1 + b2 * b2
    energy = pressure / (GAMMA - 1.0) + kinetic + 0.5 * magnetic_sq
    conserved = [density, density * v0, density * v1, density * v2, energy]
    return conserved, magnetic_sq


def flux(w, conserved, magnetic_sq, direction):
    density, v0, v1, v2, pressure, b0, b1, b2 = w
    velocity = (v0, v1, v2)
    magnetic = (b0, b1, b2)
    moving = velocity[direction]
    normal = magnetic[direction]
    total_press = pressure + 0.5 * magnetic_sq
    alignment = v0 * b0 + v1 * b1 + v2 * b2
    fast = jnp.sqrt((GAMMA * pressure + magnetic_sq) / density)
    out = [conserved[direction + 1]]
    for component in range(3):
        moment = conserved[component + 1] * moving - magnetic[component] * normal
        if component == direction:
            moment = moment + total_press
        out.append(moment)
    out.append((conserved[4] + total_press) * moving - normal * alignment)
    return out, jnp.abs(moving) + fast


def quantities(w, direction):
    conserved, magnetic_sq = cell_state(w)
    fluxes, speed = flux(w, conserved, magnetic_sq, direction)
    return conserved, fluxes, speed


def face_flux(lower, upper):
    u_low, f_low, s_low = lower
    u_up, f_up, s_up = upper
    half = 0.5 * jnp.maximum(s_low, s_up)
    return [0.5 * (f_low[i] + f_up[i]) - half * (u_up[i] - u_low[i]) for i in range(5)]


def emf(w, component):
    a, b = ((2, 3), (3, 1), (1, 2))[component]
    return -(w[a] * w[b + 4] - w[b] * w[a + 4])


def kernel(
    cells_hbm, faces_hbm, state, faces_new,
    cv, fv, first_rows, rlo, rhi, f0hi, packs, gp, th_src, gt, f1_src, f1hi, cr_src, cr, pr, e1_own, e1_src, e1f,
    load_sem, send_sem, recv_sem, ok_near, ok_wrap, ok_th,
):
    row = lax.axis_index("row")
    th = lax.axis_index("th")
    ph = lax.axis_index("ph")
    rows, ths, phs = lax.axis_size("row"), lax.axis_size("th"), lax.axis_size("ph")
    z = th * phs + ph
    depth = ths * phs
    at_bottom, at_top = row == 0, row == rows - 1
    at_north, at_south = th == 0, th == ths - 1
    first_z = z == 0
    corner_sender = (z == 2 * phs - 1) & (row > 0)

    def place(dr=0, dt=0, dp=0):
        return {"row": row + dr, "th": th + dt, "ph": lax.rem(ph + dp + phs, phs)}

    load_cells = pltpu.make_async_copy(cells_hbm, cv, load_sem.at[0])
    load_faces = pltpu.make_async_copy(faces_hbm, fv, load_sem.at[1])
    load_velocity = pltpu.make_async_copy(cells_hbm.at[2:4, :, 0:8], first_rows.at[0:2], load_sem.at[2])
    load_field = pltpu.make_async_copy(cells_hbm.at[6:8, :, 0:8], first_rows.at[2:4], load_sem.at[3])

    @pl.when(corner_sender)
    def _():
        load_velocity.start()
        load_field.start()

    load_cells.start()
    load_faces.start()

    barrier = pltpu.get_barrier_semaphore()

    def tell(semaphore, condition, target):
        @pl.when(condition)
        def _():
            pl.semaphore_signal(semaphore, inc=1, device_id=target, device_id_type=MESH)

    def told(semaphore, condition):
        @pl.when(condition)
        def _():
            pl.semaphore_wait(semaphore, 1)

    has_up, has_down = th < ths - 1, th > 0
    first_p, last_p = ph == 0, ph == phs - 1
    inner_up, inner_down = ph < phs - 1, ph > 0
    tell(barrier, row < rows - 1, place(dr=1))
    tell(barrier, row > 0, place(dr=-1))
    tell(barrier, inner_up, place(dp=1))
    tell(barrier, has_up, place(dt=1))
    tell(barrier, first_p, place(dp=-1))
    tell(barrier, (z == 0) & (row > 0), {"row": row, "th": 1, "ph": phs - 1})

    def copy(kind, src, dst, target, recv=None):
        return pltpu.make_async_remote_copy(
            src_ref=src, dst_ref=dst, send_sem=send_sem.at[kind],
            recv_sem=recv_sem.at[kind if recv is None else recv],
            device_id=target, device_id_type=MESH,
        )

    up_r, down_r = place(dr=1), place(dr=-1)
    up_t, down_t = place(dt=1), place(dt=-1)
    up_p, down_p = place(dp=1), place(dp=-1)
    origin = {"row": row, "th": th * 0, "ph": ph * 0}
    copies = {
        ROW_UP: copy(ROW_UP, cv.at[:, 3], rlo, up_r),
        ROW_DOWN: copy(ROW_DOWN, cv.at[:, 0], rhi, down_r),
        FACE_R: copy(FACE_R, fv.at[0, 0], f0hi, down_r),
        PACK_UP: copy(PACK_UP, packs.at[1], gp.at[0], up_p),
        PACK_DOWN: copy(PACK_DOWN, packs.at[0], gp.at[1], down_p),
        TH_UP: copy(TH_UP, th_src.at[1], gt.at[0], up_t),
        TH_DOWN: copy(TH_DOWN, th_src.at[0], gt.at[1], down_t),
        FACE_T: copy(FACE_T, f1_src, f1hi, down_t),
        CORNER_UP: copy(CORNER_UP, cr_src.at[1], cr.at[0], up_t),
        CORNER_DOWN: copy(CORNER_DOWN, cr_src.at[0], cr.at[1], down_t),
        PAIR_UP: copy(PAIR_UP, gp, pr.at[0], up_r),
        PAIR_DOWN: copy(PAIR_DOWN, gp, pr.at[1], down_r),
        LOW_UP: copy(LOW_UP, e1_src.at[0], e1f.at[0, 0], up_p),
        LOW_DOWN: copy(LOW_DOWN, e1_src.at[0], e1f.at[1, 0], down_p),
        HIGH_UP: copy(HIGH_UP, e1_src.at[1], e1f.at[0, 1], up_p),
        HIGH_DOWN: copy(HIGH_DOWN, e1_src.at[1], e1f.at[1, 1], down_p),
    }
    direct_left = copy(DIRECT, e1_own, e1f.at[0, 1], origin, HIGH_UP)

    def send(kind, condition=None):
        if condition is None:
            copies[kind].start()
        else:
            pl.when(condition)(copies[kind].start)

    def arrived(kind, condition=None):
        if condition is None:
            copies[kind].wait_recv()
        else:
            pl.when(condition)(copies[kind].wait_recv)

    @pl.when(corner_sender)
    def _():
        load_velocity.wait()
        load_field.wait()
        for r in range(4):
            w = [first_rows[k, r, 0:1] for k in range(4)]
            e1_own[r : r + 1] = -(w[0] * w[3] - w[1] * w[2])

    def number(*conditions):
        total = jnp.int32(0)
        for condition in conditions:
            total = total + condition.astype(jnp.int32)
        return total

    pl.semaphore_wait(barrier, number(corner_sender, has_down, last_p, row > 0, row < rows - 1, inner_down))
    pl.when(corner_sender)(direct_left.start)
    tell(ok_th, has_down, place(dt=-1))
    tell(ok_wrap, last_p, place(dp=1))
    tell(ok_near, inner_down, place(dp=-1))

    load_cells.wait()
    send(ROW_UP, row < rows - 1)
    send(ROW_DOWN, row > 0)
    for r in range(4):
        for f in range(8):
            th_src[0, f * 4 + r : f * 4 + r + 1] = cv[f, r, 0:1]
            th_src[1, f * 4 + r : f * 4 + r + 1] = cv[f, r, 15:16]
    load_faces.wait()
    send(FACE_R, row > 0)
    for r in range(4):
        f1_src[r : r + 1] = fv[1, r, 0:1]
    third = fv[2].reshape(64, 128)
    turned = jnp.concatenate([third, third], axis=0).T
    for c in range(4, 8):
        packs[0, c : c + 1] = turned[0:1]
        packs[1, c : c + 1] = turned[127:128]
    send(TH_DOWN, has_down)
    send(FACE_T, has_down)
    for c in range(4):
        turned = cv[2 * c : 2 * c + 2].reshape(128, 128).T
        packs[0, c : c + 1] = turned[0:1]
        packs[1, c : c + 1] = turned[127:128]

    @pl.when(at_bottom)
    def _():
        rlo[...] = cv[:, 0]

    @pl.when(at_top)
    def _():
        rhi[...] = cv[:, 3]
        f0hi[...] = fv[0, 3]

    def fill_polar(side, condition):
        @pl.when(condition)
        def _():
            for f in range(8):
                rows_f = th_src[side, f * 4 : f * 4 + 4]
                gt[side, f * 4 : f * 4 + 4] = -rows_f if f in (2, 7) else rows_f

    fill_polar(0, at_north)
    fill_polar(1, at_south)

    def ghost_rows(side):
        return [gt[side, f * 4 : f * 4 + 4] for f in range(8)]

    @pl.when(at_north)
    def _():
        e1_src[0] = emf(ghost_rows(0), 0)

    send(PACK_DOWN, inner_down)
    send(PACK_UP, last_p)
    send(LOW_DOWN, at_north & inner_down)
    send(LOW_UP, at_north & last_p)

    arrived(ROW_UP, row > 0)
    arrived(ROW_DOWN, row < rows - 1)
    arrived(FACE_R, row < rows - 1)
    for side, line in ((0, 0), (1, 15)):
        for k, ghost in enumerate((rlo, rhi)):
            w = [ghost[f, line : line + 1] for f in range(8)]
            cr_src[side, k : k + 1] = emf(w, 2)

    def fill_corner(side, line, condition):
        @pl.when(condition)
        def _():
            for k, ghost in enumerate((rlo, rhi)):
                w = [ghost[f, line : line + 1] for f in range(8)]
                w[2] = -w[2]
                cr[side, k : k + 1] = emf(w, 2)

    fill_corner(0, 0, at_north)
    fill_corner(1, 15, at_south)
    send(CORNER_DOWN, has_down)

    told(ok_near, inner_up)
    send(PACK_UP, inner_up)
    send(LOW_UP, at_north & inner_up)

    shape = (4, 16, 128)
    lane = lax.broadcasted_iota(jnp.int32, shape, 2)
    line = lax.broadcasted_iota(jnp.int32, shape, 1)
    own = [cv[f] for f in range(8)]

    def ahead_t(x):
        return pltpu.roll(x, 15, 1)

    def behind_t(x):
        return pltpu.roll(x, 1, 1)

    def ahead_p(x):
        return pltpu.roll(x, 127, 2)

    def behind_p(x):
        return pltpu.roll(x, 1, 2)

    low = quantities([rlo[f][None] for f in range(8)], 0)
    mid = quantities(own, 0)
    high = quantities([rhi[f][None] for f in range(8)], 0)

    def tall(a, b, c):
        return jnp.concatenate([a, b, c], axis=0)

    u6 = [tall(low[0][i], mid[0][i], high[0][i]) for i in range(5)]
    g6 = [tall(low[1][i], mid[1][i], high[1][i]) for i in range(5)]
    s6 = tall(low[2], mid[2], high[2])
    face = face_flux(([u[:-1] for u in u6], [g[:-1] for g in g6], s6[:-1]), ([u[1:] for u in u6], [g[1:] for g in g6], s6[1:]))
    for i in range(5):
        state[i] = mid[0][i] - STEP * (face[i][1:] - face[i][:-1])

    told(ok_wrap, first_p)
    send(PACK_DOWN, first_p)
    send(LOW_DOWN, at_north & first_p)

    def send_up(condition):
        told(ok_th, condition)
        send(TH_UP, condition)
        send(CORNER_UP, condition)

    send_up(has_up & last_p)

    arrived(PACK_DOWN)
    arrived(PACK_UP)
    send(PAIR_UP, row < rows - 1)
    send(PAIR_DOWN, row > 0)
    columns = jnp.concatenate([gp[0], gp[1]], axis=0).T

    def column(side, c, half):
        col = columns[half * 64 : half * 64 + 64, side * 8 + c : side * 8 + c + 1]
        return jnp.broadcast_to(col, (64, 128)).reshape(shape)

    left, right = lane == 0, lane == 127
    beside = [
        jnp.where(left, column(0, f // 2, f % 2), jnp.where(right, column(1, f // 2, f % 2), own[f]))
        for f in range(8)
    ]
    upper_third = column(1, 4, 0)
    e1_beside, e2_beside = emf(beside, 0), emf(beside, 1)

    def apply(direction, outer, ahead, behind, is_low, is_high):
        mine = quantities(own, direction)
        edge = quantities(outer, direction)

        def shifted(a, b):
            return jnp.where(is_high, b, ahead(a))

        above = (
            [shifted(mine[0][i], edge[0][i]) for i in range(5)],
            [shifted(mine[1][i], edge[1][i]) for i in range(5)],
            shifted(mine[2], edge[2]),
        )
        upper = face_flux(mine, above)
        lower = face_flux(edge, mine)
        for i in range(5):
            below = jnp.where(is_low, lower[i], behind(upper[i]))
            state[i] = state[i] - STEP * (upper[i] - below)

    apply(2, beside, ahead_p, behind_p, left, right)
    send_up(has_up & jnp.logical_not(last_p))

    arrived(TH_UP, th > 0)

    @pl.when(th > 0)
    def _():
        e1_src[0] = emf(ghost_rows(0), 0)

    send(LOW_UP, th > 0)
    send(LOW_DOWN, th > 0)
    arrived(TH_DOWN, th < ths - 1)
    arrived(FACE_T, th < ths - 1)
    e1_src[1] = emf(ghost_rows(1), 0)
    high_up = (z != phs - 1) | (row == 0)
    send(HIGH_UP, high_up)
    send(HIGH_DOWN)

    north, south = line == 0, line == 15

    def spread(ref, *index):
        return jnp.concatenate([jnp.broadcast_to(ref[index + (slice(start, start + 1),)], (16, 128))[None] for start in spread.rows], axis=0)

    def polar(f):
        spread.rows = [f * 4 + r for r in range(4)]
        return jnp.where(north, spread(gt, 0), jnp.where(south, spread(gt, 1), own[f]))

    outside = [polar(f) for f in range(8)]
    apply(1, outside, ahead_t, behind_t, north, south)
    e1_outside, e3_outside = emf(outside, 0), emf(outside, 2)

    arrived(CORNER_UP, th > 0)
    arrived(CORNER_DOWN, th < ths - 1)
    arrived(PAIR_UP, row > 0)
    arrived(PAIR_DOWN, row < rows - 1)

    def pair_emf(ref, *index):
        rows8 = ref[index] if index else ref[...]
        return -(rows8[1:2] * rows8[2:3] - rows8[0:1] * rows8[3:4])

    pair_rows = [pair_emf(gp, 0), pair_emf(gp, 1), pair_emf(pr, 0, 0), pair_emf(pr, 0, 1), pair_emf(pr, 1, 0), pair_emf(pr, 1, 1)]
    pair_columns = jnp.concatenate(pair_rows + [pair_rows[0], pair_rows[0]], axis=0).T

    def pair_ghost(side):
        lanes = lane[:1]
        parts = []
        for k in range(2):
            near = pair_columns[64:80, k : k + 1] if side == 0 else pair_columns[112:128, k : k + 1]
            far_col = pair_columns[112:128, 2 + k : 3 + k] if side == 0 else pair_columns[64:80, 4 + k : 5 + k]
            edge = at_bottom if side == 0 else at_top
            parts.append(jnp.broadcast_to(jnp.where(edge, near, far_col), (16, 128))[None])
        return jnp.where(lanes == 0, parts[0], parts[1])

    def corner_ghost(k):
        a = jnp.broadcast_to(cr[0, k : k + 1], (16, 128))[None]
        b = jnp.broadcast_to(cr[1, k : k + 1], (16, 128))[None]
        return jnp.where(line[:1] == 0, a, b)

    low_w = [rlo[f][None] for f in range(8)]
    high_w = [rhi[f][None] for f in range(8)]
    e1 = emf(own, 0)
    e2 = tall(emf(low_w, 1), emf(own, 1), emf(high_w, 1))
    e3 = tall(emf(low_w, 2), emf(own, 2), emf(high_w, 2))
    e2_side = tall(pair_ghost(0), e2_beside, pair_ghost(1))
    e3_side = tall(corner_ghost(0), e3_outside, corner_ghost(1))

    six = (6, 16, 128)
    lane6 = lax.broadcasted_iota(jnp.int32, six, 2)
    line6 = lax.broadcasted_iota(jnp.int32, six, 1)
    across_t = jnp.where(line6 == 15, e3_side, ahead_t(e3)) - jnp.where(line6 == 0, e3_side, behind_t(e3))
    across_p = jnp.where(lane6 == 127, e2_side, ahead_p(e2)) - jnp.where(lane6 == 0, e2_side, behind_p(e2))
    curl = across_t - across_p
    new_first = fv[0] - QUARTER * (curl[:4] + curl[1:5])
    new_last = f0hi[...] - QUARTER * (curl[4] + curl[5])
    faces_new[0] = new_first
    last = jnp.where(at_top, new_first[3], new_last)
    state[5] = 0.5 * (new_first + jnp.concatenate([new_first[1:], last[None]], axis=0))

    zero = jnp.zeros(shape, jnp.float32)
    curl = (e2[2:] - e2[:-2]) - (
        jnp.where(south, e1_outside, ahead_t(e1)) - jnp.where(north, e1_outside, behind_t(e1))
    )
    curl_beside = (e2_side[2:] - e2_side[:-2]) - (
        jnp.where(south, zero, ahead_t(e1_beside)) - jnp.where(north, zero, behind_t(e1_beside))
    )
    new_third = fv[2] - QUARTER * (curl + jnp.where(left, curl_beside, behind_p(curl)))
    new_upper = upper_third - QUARTER * (curl + curl_beside)
    faces_new[2] = new_third
    state[7] = 0.5 * (new_third + jnp.where(right, new_upper, ahead_p(new_third)))

    curl = (
        jnp.where(right, e1_beside, ahead_p(e1)) - jnp.where(left, e1_beside, behind_p(e1))
    ) - (e3[2:] - e3[:-2])
    curl_outside = (
        jnp.where(right, zero, ahead_p(e1_outside)) - jnp.where(left, zero, behind_p(e1_outside))
    ) - (e3_side[2:] - e3_side[:-2])
    new_second = fv[1] - QUARTER * (curl + jnp.where(north, curl_outside, behind_t(curl)))
    spread.rows = [0, 1, 2, 3]
    new_upper = spread(f1hi) - QUARTER * (curl + curl_outside)
    new_upper = jnp.where(at_south, 0.0, new_upper)
    faces_new[1] = new_second
    state[6] = 0.5 * (new_second + jnp.where(south, new_upper, ahead_t(new_second)))

    arrived(LOW_UP)
    arrived(LOW_DOWN)
    arrived(HIGH_DOWN)
    arrived(HIGH_UP)
    lane4 = lax.broadcasted_iota(jnp.int32, (4, 128), 1)

    def corner_rows(k):
        a = jnp.where(lane4 == 0, pltpu.roll(e1f[0, k], 1, 1), 0.0)
        b = jnp.where(lane4 == 127, pltpu.roll(e1f[1, k], 127, 1), 0.0)
        return QUARTER * a, QUARTER * b

    a_low, b_low = corner_rows(0)
    a_high, b_high = corner_rows(1)
    keep = jnp.where(at_south, 0.0, 0.5)
    for r in range(4):
        a, b = a_low[r : r + 1], b_low[r : r + 1]
        faces_new[1, r, 0:1] = faces_new[1, r, 0:1] - (b - a)
        state[6, r, 0:1] = state[6, r, 0:1] - 0.5 * (b - a)
        faces_new[2, r, 0:1] = faces_new[2, r, 0:1] - a
        state[7, r, 0:1] = state[7, r, 0:1] - 0.5 * (a + b)
        a, b = a_high[r : r + 1], b_high[r : r + 1]
        state[6, r, 15:16] = state[6, r, 15:16] - keep * (b - a)
        faces_new[2, r, 15:16] = faces_new[2, r, 15:16] + a
        state[7, r, 15:16] = state[7, r, 15:16] + 0.5 * (a + b)

    for kind, condition in (
        (ROW_UP, row < rows - 1), (ROW_DOWN, row > 0), (FACE_R, row > 0), (PACK_UP, None), (PACK_DOWN, None),
        (TH_UP, th < ths - 1), (TH_DOWN, th > 0), (FACE_T, th > 0), (CORNER_UP, th < ths - 1), (CORNER_DOWN, th > 0),
        (PAIR_UP, row < rows - 1), (PAIR_DOWN, row > 0), (LOW_UP, None), (LOW_DOWN, None),
        (HIGH_UP, high_up), (HIGH_DOWN, None),
    ):
        if condition is None:
            copies[kind].wait_send()
        else:
            pl.when(condition)(copies[kind].wait_send)
    pl.when(corner_sender)(direct_left.wait_send)


def write_out(state, faces_new, state_hbm, faces_hbm, sem):
    copies = [
        pltpu.make_async_copy(state, state_hbm, sem.at[0]),
        pltpu.make_async_copy(faces_new, faces_hbm, sem.at[1]),
    ]
    for copy in copies:
        copy.start()
    for copy in copies:
        copy.wait()


def on_device(cells, faces):
    f32 = jnp.float32
    shapes = ((8, 4, 16, 128), (3, 4, 16, 128))
    outputs = pl.pallas_call(
        kernel,
        out_shape=tuple(pltpu.VMEM(shape, f32) for shape in shapes),
        in_specs=[pl.BlockSpec(memory_space=pl.ANY)] * 2,
        out_specs=(pl.BlockSpec(memory_space=pltpu.VMEM),) * 2,
        scratch_shapes=[
            pltpu.VMEM((8, 4, 16, 128), f32),
            pltpu.VMEM((3, 4, 16, 128), f32),
            pltpu.VMEM((4, 4, 8, 128), f32),
            pltpu.VMEM((8, 16, 128), f32),
            pltpu.VMEM((8, 16, 128), f32),
            pltpu.VMEM((16, 128), f32),
            pltpu.VMEM((2, 8, 128), f32),
            pltpu.VMEM((2, 8, 128), f32),
            pltpu.VMEM((2, 32, 128), f32),
            pltpu.VMEM((2, 32, 128), f32),
            pltpu.VMEM((4, 128), f32),
            pltpu.VMEM((4, 128), f32),
            pltpu.VMEM((2, 2, 128), f32),
            pltpu.VMEM((2, 2, 128), f32),
            pltpu.VMEM((2, 2, 8, 128), f32),
            pltpu.VMEM((4, 128), f32),
            pltpu.VMEM((2, 4, 128), f32),
            pltpu.VMEM((2, 2, 4, 128), f32),
            pltpu.SemaphoreType.DMA((4,)),
            pltpu.SemaphoreType.DMA((17,)),
            pltpu.SemaphoreType.DMA((17,)),
            pltpu.SemaphoreType.REGULAR,
            pltpu.SemaphoreType.REGULAR,
            pltpu.SemaphoreType.REGULAR,
        ],
        name="section",
        compiler_params=pltpu.CompilerParams(collective_id=0, has_side_effects=True),
    )(cells, faces)
    return pl.pallas_call(
        write_out,
        out_shape=tuple(jax.ShapeDtypeStruct(shape, f32) for shape in shapes),
        in_specs=[pl.BlockSpec(memory_space=pltpu.VMEM)] * 2,
        out_specs=(pl.BlockSpec(memory_space=pl.ANY),) * 2,
        scratch_shapes=[pltpu.SemaphoreType.DMA((2,))],
        name="write_out",
    )(*(pltpu.with_memory_space_constraint(x, pltpu.VMEM) for x in outputs))


def solution(mesh):
    spec = P(None, "row", "th", "ph")
    return jax.shard_map(on_device, mesh=mesh, in_specs=(spec, spec), out_specs=(spec, spec), check_vma=False)
```

```python
import jax
import jax.numpy as jnp
from jax import lax
from jax.experimental import pallas as pl
from jax.experimental.pallas import tpu as pltpu
from jax.sharding import PartitionSpec as P

MESH = pl.DeviceIdType.MESH
STEP = 0.05
QUARTER = 0.0125
GAMMA = 5.0 / 3.0

ROW_UP, ROW_DOWN, FACE_R, PACK_UP, PACK_DOWN, TH_UP, TH_DOWN, FACE_T = range(8)
CORNER_UP, CORNER_DOWN, PAIR_UP, PAIR_DOWN, LOW_UP, LOW_DOWN, HIGH_UP, HIGH_DOWN = range(8, 16)
E1_UP, E1_DOWN, DIRECT = 16, 17, 18


def cell_state(w):
    density, v0, v1, v2, pressure, b0, b1, b2 = w
    kinetic = 0.5 * density * (v0 * v0 + v1 * v1 + v2 * v2)
    magnetic_sq = b0 * b0 + b1 * b1 + b2 * b2
    energy = pressure / (GAMMA - 1.0) + kinetic + 0.5 * magnetic_sq
    conserved = [density, density * v0, density * v1, density * v2, energy]
    return conserved, magnetic_sq


def flux(w, conserved, magnetic_sq, direction):
    density, v0, v1, v2, pressure, b0, b1, b2 = w
    velocity = (v0, v1, v2)
    magnetic = (b0, b1, b2)
    moving = velocity[direction]
    normal = magnetic[direction]
    total_press = pressure + 0.5 * magnetic_sq
    alignment = v0 * b0 + v1 * b1 + v2 * b2
    fast = jnp.sqrt((GAMMA * pressure + magnetic_sq) / density)
    out = [conserved[direction + 1]]
    for component in range(3):
        moment = conserved[component + 1] * moving - magnetic[component] * normal
        if component == direction:
            moment = moment + total_press
        out.append(moment)
    out.append((conserved[4] + total_press) * moving - normal * alignment)
    return out, jnp.abs(moving) + fast


def quantities(w, direction):
    conserved, magnetic_sq = cell_state(w)
    fluxes, speed = flux(w, conserved, magnetic_sq, direction)
    return conserved, fluxes, speed


def face_flux(lower, upper):
    u_low, f_low, s_low = lower
    u_up, f_up, s_up = upper
    half = 0.5 * jnp.maximum(s_low, s_up)
    return [0.5 * (f_low[i] + f_up[i]) - half * (u_up[i] - u_low[i]) for i in range(5)]


def emf(w, component):
    a, b = ((2, 3), (3, 1), (1, 2))[component]
    return -(w[a] * w[b + 4] - w[b] * w[a + 4])


def kernel(
    cells_hbm, faces_hbm, state, faces_new,
    cv, fv, first_rows, rlo, rhi, f0hi, packs, gp, th_src, gt, f1_src, f1hi, cr_src, cr, pr, e1_corner, e1_src, e1g, e1f,
    load_sem, send_sem, recv_sem, ok_near, ok_wrap, ok_th, ok_side, ok_row,
):
    row = lax.axis_index("row")
    th = lax.axis_index("th")
    ph = lax.axis_index("ph")
    rows, ths, phs = lax.axis_size("row"), lax.axis_size("th"), lax.axis_size("ph")
    z = th * phs + ph
    depth = ths * phs
    at_bottom, at_top = row == 0, row == rows - 1
    at_north, at_south = th == 0, th == ths - 1
    first_z = z == 0
    corner_place = z == 2 * phs - 1
    beside_corner = z == 2 * phs - 2
    corner_sender = corner_place & (row > 0)

    def place(dr=0, dt=0, dp=0):
        return {"row": row + dr, "th": th + dt, "ph": lax.rem(ph + dp + phs, phs)}

    load_cells = pltpu.make_async_copy(cells_hbm, cv, load_sem.at[0])
    load_faces = pltpu.make_async_copy(faces_hbm, fv, load_sem.at[1])
    load_velocity = pltpu.make_async_copy(cells_hbm.at[2:4, :, 0:8], first_rows.at[0:2], load_sem.at[2])
    load_field = pltpu.make_async_copy(cells_hbm.at[6:8, :, 0:8], first_rows.at[2:4], load_sem.at[3])

    @pl.when(corner_sender)
    def _():
        load_velocity.start()
        load_field.start()

    load_cells.start()
    load_faces.start()

    barrier = pltpu.get_barrier_semaphore()

    def tell(semaphore, condition, target):
        @pl.when(condition)
        def _():
            pl.semaphore_signal(semaphore, inc=1, device_id=target, device_id_type=MESH)

    def told(semaphore, condition):
        @pl.when(condition)
        def _():
            pl.semaphore_wait(semaphore, 1)

    has_up, has_down = th < ths - 1, th > 0
    first_p, last_p = ph == 0, ph == phs - 1
    inner_up, inner_down = ph < phs - 1, ph > 0
    row_up, row_down = row < rows - 1, row > 0
    plain = jnp.logical_not(corner_place)
    tell(barrier, row_up & plain, place(dr=1))
    tell(barrier, row_down & plain, place(dr=-1))
    tell(barrier, corner_place, place(dp=-1))
    tell(barrier, inner_up, place(dp=1))
    tell(barrier, has_up, place(dt=1))
    tell(barrier, first_p, place(dp=-1))
    tell(barrier, (z == 0) & (row > 0), {"row": row, "th": 1, "ph": phs - 1})

    def copy(kind, src, dst, target, recv=None):
        return pltpu.make_async_remote_copy(
            src_ref=src, dst_ref=dst, send_sem=send_sem.at[kind],
            recv_sem=recv_sem.at[kind if recv is None else recv],
            device_id=target, device_id_type=MESH,
        )

    up_r, down_r = place(dr=1), place(dr=-1)
    up_t, down_t = place(dt=1), place(dt=-1)
    up_p, down_p = place(dp=1), place(dp=-1)
    origin = {"row": row, "th": th * 0, "ph": ph * 0}
    copies = {
        ROW_UP: copy(ROW_UP, cv.at[:, 3], rlo, up_r),
        ROW_DOWN: copy(ROW_DOWN, cv.at[:, 0], rhi, down_r),
        FACE_R: copy(FACE_R, fv.at[0, 0], f0hi, down_r),
        PACK_UP: copy(PACK_UP, packs.at[1], gp.at[0], up_p),
        PACK_DOWN: copy(PACK_DOWN, packs.at[0], gp.at[1], down_p),
        TH_UP: copy(TH_UP, th_src.at[1], gt.at[0], up_t),
        TH_DOWN: copy(TH_DOWN, th_src.at[0], gt.at[1], down_t),
        FACE_T: copy(FACE_T, f1_src, f1hi, down_t),
        CORNER_UP: copy(CORNER_UP, cr_src.at[1], cr.at[0], up_t),
        CORNER_DOWN: copy(CORNER_DOWN, cr_src.at[0], cr.at[1], down_t),
        PAIR_UP: copy(PAIR_UP, gp, pr.at[0], up_r),
        PAIR_DOWN: copy(PAIR_DOWN, gp, pr.at[1], down_r),
        E1_UP: copy(E1_UP, e1_src.at[1], e1g.at[0], up_t),
        E1_DOWN: copy(E1_DOWN, e1_src.at[0], e1g.at[1], down_t),
        LOW_UP: copy(LOW_UP, e1g.at[0], e1f.at[0, 0], up_p),
        LOW_DOWN: copy(LOW_DOWN, e1g.at[0], e1f.at[1, 0], down_p),
        HIGH_UP: copy(HIGH_UP, e1g.at[1], e1f.at[0, 1], up_p),
        HIGH_DOWN: copy(HIGH_DOWN, e1g.at[1], e1f.at[1, 1], down_p),
    }
    direct_left = copy(DIRECT, e1_corner, e1f.at[0, 1], origin, HIGH_UP)

    def send(kind, condition=None):
        if condition is None:
            copies[kind].start()
        else:
            pl.when(condition)(copies[kind].start)

    def arrived(kind, condition=None):
        if condition is None:
            copies[kind].wait_recv()
        else:
            pl.when(condition)(copies[kind].wait_recv)

    @pl.when(corner_sender)
    def _():
        load_velocity.wait()
        load_field.wait()
        for r in range(4):
            w = [first_rows[k, r, 0:1] for k in range(4)]
            e1_corner[r : r + 1] = -(w[0] * w[3] - w[1] * w[2])

    def number(*conditions):
        total = jnp.int32(0)
        for condition in conditions:
            total = total + condition.astype(jnp.int32)
        return total

    pl.semaphore_wait(
        barrier,
        number(corner_sender, has_down, last_p, row_down & plain, row_up & plain, inner_down, beside_corner),
    )
    pl.when(corner_sender)(direct_left.start)
    tell(ok_th, has_down, place(dt=-1))
    tell(ok_wrap, last_p, place(dp=1))
    tell(ok_near, inner_down & plain, place(dp=-1))
    tell(ok_side, beside_corner & row_up, place(dr=1))
    tell(ok_side, beside_corner & row_down, place(dr=-1))

    load_cells.wait()
    send(ROW_UP, row_up & plain)
    send(ROW_DOWN, row_down & plain)
    for r in range(4):
        for f in range(8):
            th_src[0, f * 4 + r : f * 4 + r + 1] = cv[f, r, 0:1]
            th_src[1, f * 4 + r : f * 4 + r + 1] = cv[f, r, 15:16]
    for side in range(2):
        e1_src[side] = emf([th_src[side, f * 4 : f * 4 + 4] for f in range(8)], 0)
    send(E1_DOWN, has_down)
    load_faces.wait()
    send(FACE_R, row_down & plain)
    for r in range(4):
        f1_src[r : r + 1] = fv[1, r, 0:1]
    third = fv[2].reshape(64, 128)
    turned = jnp.concatenate([third, third], axis=0).T
    for c in range(4, 8):
        packs[0, c : c + 1] = turned[0:1]
        packs[1, c : c + 1] = turned[127:128]
    send(TH_DOWN, has_down)
    send(FACE_T, has_down)
    for c in range(4):
        turned = cv[2 * c : 2 * c + 2].reshape(128, 128).T
        packs[0, c : c + 1] = turned[0:1]
        packs[1, c : c + 1] = turned[127:128]

    @pl.when(at_bottom)
    def _():
        rlo[...] = cv[:, 0]

    @pl.when(at_top)
    def _():
        rhi[...] = cv[:, 3]
        f0hi[...] = fv[0, 3]

    def fill_polar(side, condition):
        @pl.when(condition)
        def _():
            for f in range(8):
                rows_f = th_src[side, f * 4 : f * 4 + 4]
                gt[side, f * 4 : f * 4 + 4] = -rows_f if f in (2, 7) else rows_f

    fill_polar(0, at_north)
    fill_polar(1, at_south)

    def ghost_rows(side):
        return [gt[side, f * 4 : f * 4 + 4] for f in range(8)]

    @pl.when(at_north)
    def _():
        e1g[0] = emf(ghost_rows(0), 0)

    @pl.when(at_south)
    def _():
        e1g[1] = emf(ghost_rows(1), 0)

    send(PACK_DOWN, inner_down)
    send(PACK_UP, last_p)
    send(LOW_DOWN, at_north & inner_down)
    send(LOW_UP, at_north & last_p)

    @pl.when(beside_corner)
    def _():
        pl.semaphore_wait(ok_side, number(row_up, row_down))

    tell(ok_row, beside_corner, place(dp=1))
    told(ok_row, corner_place)
    send(ROW_UP, row_up & corner_place)
    send(ROW_DOWN, row_down & corner_place)
    send(FACE_R, row_down & corner_place)

    arrived(ROW_UP, row > 0)
    arrived(ROW_DOWN, row < rows - 1)
    arrived(FACE_R, row < rows - 1)
    for side, line in ((0, 0), (1, 15)):
        for k, ghost in enumerate((rlo, rhi)):
            w = [ghost[f, line : line + 1] for f in range(8)]
            cr_src[side, k : k + 1] = emf(w, 2)

    def fill_corner(side, line, condition):
        @pl.when(condition)
        def _():
            for k, ghost in enumerate((rlo, rhi)):
                w = [ghost[f, line : line + 1] for f in range(8)]
                w[2] = -w[2]
                cr[side, k : k + 1] = emf(w, 2)

    fill_corner(0, 0, at_north)
    fill_corner(1, 15, at_south)
    send(CORNER_DOWN, has_down)

    told(ok_near, inner_up & jnp.logical_not(beside_corner))
    send(PACK_UP, inner_up)
    send(LOW_UP, at_north & inner_up)

    shape = (4, 16, 128)
    lane = lax.broadcasted_iota(jnp.int32, shape, 2)
    line = lax.broadcasted_iota(jnp.int32, shape, 1)
    own = [cv[f] for f in range(8)]

    def ahead_t(x):
        return pltpu.roll(x, 15, 1)

    def behind_t(x):
        return pltpu.roll(x, 1, 1)

    def ahead_p(x):
        return pltpu.roll(x, 127, 2)

    def behind_p(x):
        return pltpu.roll(x, 1, 2)

    low = quantities([rlo[f][None] for f in range(8)], 0)
    mid = quantities(own, 0)
    high = quantities([rhi[f][None] for f in range(8)], 0)

    def tall(a, b, c):
        return jnp.concatenate([a, b, c], axis=0)

    u6 = [tall(low[0][i], mid[0][i], high[0][i]) for i in range(5)]
    g6 = [tall(low[1][i], mid[1][i], high[1][i]) for i in range(5)]
    s6 = tall(low[2], mid[2], high[2])
    face = face_flux(([u[:-1] for u in u6], [g[:-1] for g in g6], s6[:-1]), ([u[1:] for u in u6], [g[1:] for g in g6], s6[1:]))
    for i in range(5):
        state[i] = mid[0][i] - STEP * (face[i][1:] - face[i][:-1])

    told(ok_wrap, first_p)
    send(PACK_DOWN, first_p)
    send(LOW_DOWN, at_north & first_p)

    def send_up(condition):
        told(ok_th, condition)
        send(E1_UP, condition)
        send(TH_UP, condition)
        send(CORNER_UP, condition)

    send_up(has_up & last_p)

    arrived(PACK_DOWN)
    arrived(PACK_UP)
    send(PAIR_UP, row < rows - 1)
    send(PAIR_DOWN, row > 0)
    columns = jnp.concatenate([gp[0], gp[1]], axis=0).T

    def column(side, c, half):
        col = columns[half * 64 : half * 64 + 64, side * 8 + c : side * 8 + c + 1]
        return jnp.broadcast_to(col, (64, 128)).reshape(shape)

    left, right = lane == 0, lane == 127
    beside = [
        jnp.where(left, column(0, f // 2, f % 2), jnp.where(right, column(1, f // 2, f % 2), own[f]))
        for f in range(8)
    ]
    upper_third = column(1, 4, 0)
    e1_beside, e2_beside = emf(beside, 0), emf(beside, 1)

    def apply(direction, outer, ahead, behind, is_low, is_high):
        mine = quantities(own, direction)
        edge = quantities(outer, direction)

        def shifted(a, b):
            return jnp.where(is_high, b, ahead(a))

        above = (
            [shifted(mine[0][i], edge[0][i]) for i in range(5)],
            [shifted(mine[1][i], edge[1][i]) for i in range(5)],
            shifted(mine[2], edge[2]),
        )
        upper = face_flux(mine, above)
        lower = face_flux(edge, mine)
        for i in range(5):
            below = jnp.where(is_low, lower[i], behind(upper[i]))
            state[i] = state[i] - STEP * (upper[i] - below)

    apply(2, beside, ahead_p, behind_p, left, right)
    send_up(has_up & jnp.logical_not(last_p))

    arrived(E1_UP, has_down)
    send(LOW_UP, has_down)
    send(LOW_DOWN, has_down)
    arrived(E1_DOWN, has_up)
    high_up = (z != phs - 1) | (row == 0)
    send(HIGH_UP, high_up)
    send(HIGH_DOWN)

    arrived(TH_UP, has_down)
    arrived(TH_DOWN, has_up)
    arrived(FACE_T, has_up)

    north, south = line == 0, line == 15

    def spread(ref, *index):
        return jnp.concatenate([jnp.broadcast_to(ref[index + (slice(start, start + 1),)], (16, 128))[None] for start in spread.rows], axis=0)

    def polar(f):
        spread.rows = [f * 4 + r for r in range(4)]
        return jnp.where(north, spread(gt, 0), jnp.where(south, spread(gt, 1), own[f]))

    outside = [polar(f) for f in range(8)]
    apply(1, outside, ahead_t, behind_t, north, south)
    e1_outside, e3_outside = emf(outside, 0), emf(outside, 2)

    arrived(CORNER_UP, th > 0)
    arrived(CORNER_DOWN, th < ths - 1)
    arrived(PAIR_UP, row > 0)
    arrived(PAIR_DOWN, row < rows - 1)

    def pair_emf(ref, *index):
        rows8 = ref[index] if index else ref[...]
        return -(rows8[1:2] * rows8[2:3] - rows8[0:1] * rows8[3:4])

    pair_rows = [pair_emf(gp, 0), pair_emf(gp, 1), pair_emf(pr, 0, 0), pair_emf(pr, 0, 1), pair_emf(pr, 1, 0), pair_emf(pr, 1, 1)]
    pair_columns = jnp.concatenate(pair_rows + [pair_rows[0], pair_rows[0]], axis=0).T

    def pair_ghost(side):
        lanes = lane[:1]
        parts = []
        for k in range(2):
            near = pair_columns[64:80, k : k + 1] if side == 0 else pair_columns[112:128, k : k + 1]
            far_col = pair_columns[112:128, 2 + k : 3 + k] if side == 0 else pair_columns[64:80, 4 + k : 5 + k]
            edge = at_bottom if side == 0 else at_top
            parts.append(jnp.broadcast_to(jnp.where(edge, near, far_col), (16, 128))[None])
        return jnp.where(lanes == 0, parts[0], parts[1])

    def corner_ghost(k):
        a = jnp.broadcast_to(cr[0, k : k + 1], (16, 128))[None]
        b = jnp.broadcast_to(cr[1, k : k + 1], (16, 128))[None]
        return jnp.where(line[:1] == 0, a, b)

    low_w = [rlo[f][None] for f in range(8)]
    high_w = [rhi[f][None] for f in range(8)]
    e1 = emf(own, 0)
    e2 = tall(emf(low_w, 1), emf(own, 1), emf(high_w, 1))
    e3 = tall(emf(low_w, 2), emf(own, 2), emf(high_w, 2))
    e2_side = tall(pair_ghost(0), e2_beside, pair_ghost(1))
    e3_side = tall(corner_ghost(0), e3_outside, corner_ghost(1))

    six = (6, 16, 128)
    lane6 = lax.broadcasted_iota(jnp.int32, six, 2)
    line6 = lax.broadcasted_iota(jnp.int32, six, 1)
    across_t = jnp.where(line6 == 15, e3_side, ahead_t(e3)) - jnp.where(line6 == 0, e3_side, behind_t(e3))
    across_p = jnp.where(lane6 == 127, e2_side, ahead_p(e2)) - jnp.where(lane6 == 0, e2_side, behind_p(e2))
    curl = across_t - across_p
    new_first = fv[0] - QUARTER * (curl[:4] + curl[1:5])
    new_last = f0hi[...] - QUARTER * (curl[4] + curl[5])
    faces_new[0] = new_first
    last = jnp.where(at_top, new_first[3], new_last)
    state[5] = 0.5 * (new_first + jnp.concatenate([new_first[1:], last[None]], axis=0))

    zero = jnp.zeros(shape, jnp.float32)
    curl = (e2[2:] - e2[:-2]) - (
        jnp.where(south, e1_outside, ahead_t(e1)) - jnp.where(north, e1_outside, behind_t(e1))
    )
    curl_beside = (e2_side[2:] - e2_side[:-2]) - (
        jnp.where(south, zero, ahead_t(e1_beside)) - jnp.where(north, zero, behind_t(e1_beside))
    )
    new_third = fv[2] - QUARTER * (curl + jnp.where(left, curl_beside, behind_p(curl)))
    new_upper = upper_third - QUARTER * (curl + curl_beside)
    faces_new[2] = new_third
    state[7] = 0.5 * (new_third + jnp.where(right, new_upper, ahead_p(new_third)))

    curl = (
        jnp.where(right, e1_beside, ahead_p(e1)) - jnp.where(left, e1_beside, behind_p(e1))
    ) - (e3[2:] - e3[:-2])
    curl_outside = (
        jnp.where(right, zero, ahead_p(e1_outside)) - jnp.where(left, zero, behind_p(e1_outside))
    ) - (e3_side[2:] - e3_side[:-2])
    new_second = fv[1] - QUARTER * (curl + jnp.where(north, curl_outside, behind_t(curl)))
    spread.rows = [0, 1, 2, 3]
    new_upper = spread(f1hi) - QUARTER * (curl + curl_outside)
    new_upper = jnp.where(at_south, 0.0, new_upper)
    faces_new[1] = new_second
    state[6] = 0.5 * (new_second + jnp.where(south, new_upper, ahead_t(new_second)))

    for kind, condition in (
        (ROW_UP, row_up), (ROW_DOWN, row_down), (FACE_R, row_down), (PACK_UP, None), (PACK_DOWN, None),
        (TH_UP, has_up), (TH_DOWN, has_down), (FACE_T, has_down), (CORNER_UP, has_up), (CORNER_DOWN, has_down),
        (PAIR_UP, row_up), (PAIR_DOWN, row_down), (LOW_UP, None), (LOW_DOWN, None),
        (HIGH_UP, high_up), (HIGH_DOWN, None), (E1_UP, has_up), (E1_DOWN, has_down),
    ):
        if condition is None:
            copies[kind].wait_send()
        else:
            pl.when(condition)(copies[kind].wait_send)
    pl.when(corner_sender)(direct_left.wait_send)

    lane4 = lax.broadcasted_iota(jnp.int32, (4, 128), 1)

    def from_left(k):
        return QUARTER * jnp.where(lane4 == 0, pltpu.roll(e1f[0, k], 1, 1), 0.0)

    def from_right(k):
        return QUARTER * jnp.where(lane4 == 127, pltpu.roll(e1f[1, k], 127, 1), 0.0)

    keep = jnp.where(at_south, 0.0, 0.5)

    def adjust(ref, r, place_row, amount):
        ref[r, place_row : place_row + 1] = ref[r, place_row : place_row + 1] + amount

    arrived(LOW_UP)
    arrived(LOW_DOWN)
    a_low, b_low = from_left(0), from_right(0)
    for r in range(4):
        a, b = a_low[r : r + 1], b_low[r : r + 1]
        adjust(faces_new.at[1], r, 0, a - b)
        adjust(state.at[6], r, 0, 0.5 * (a - b))
        adjust(faces_new.at[2], r, 0, -a)
        adjust(state.at[7], r, 0, -0.5 * (a + b))
    arrived(HIGH_DOWN)
    b_high = from_right(1)
    for r in range(4):
        b = b_high[r : r + 1]
        adjust(state.at[6], r, 15, -keep * b)
        adjust(state.at[7], r, 15, 0.5 * b)
    arrived(HIGH_UP)
    a_high = from_left(1)
    for r in range(4):
        a = a_high[r : r + 1]
        adjust(state.at[6], r, 15, keep * a)
        adjust(faces_new.at[2], r, 15, a)
        adjust(state.at[7], r, 15, 0.5 * a)


def write_out(state, faces_new, state_hbm, faces_hbm, sem):
    copies = [
        pltpu.make_async_copy(state, state_hbm, sem.at[0]),
        pltpu.make_async_copy(faces_new, faces_hbm, sem.at[1]),
    ]
    for copy in copies:
        copy.start()
    for copy in copies:
        copy.wait()


def on_device(cells, faces):
    f32 = jnp.float32
    shapes = ((8, 4, 16, 128), (3, 4, 16, 128))
    outputs = pl.pallas_call(
        kernel,
        out_shape=tuple(pltpu.VMEM(shape, f32) for shape in shapes),
        in_specs=[pl.BlockSpec(memory_space=pl.ANY)] * 2,
        out_specs=(pl.BlockSpec(memory_space=pltpu.VMEM),) * 2,
        scratch_shapes=[
            pltpu.VMEM((8, 4, 16, 128), f32),
            pltpu.VMEM((3, 4, 16, 128), f32),
            pltpu.VMEM((4, 4, 8, 128), f32),
            pltpu.VMEM((8, 16, 128), f32),
            pltpu.VMEM((8, 16, 128), f32),
            pltpu.VMEM((16, 128), f32),
            pltpu.VMEM((2, 8, 128), f32),
            pltpu.VMEM((2, 8, 128), f32),
            pltpu.VMEM((2, 32, 128), f32),
            pltpu.VMEM((2, 32, 128), f32),
            pltpu.VMEM((4, 128), f32),
            pltpu.VMEM((4, 128), f32),
            pltpu.VMEM((2, 2, 128), f32),
            pltpu.VMEM((2, 2, 128), f32),
            pltpu.VMEM((2, 2, 8, 128), f32),
            pltpu.VMEM((4, 128), f32),
            pltpu.VMEM((2, 4, 128), f32),
            pltpu.VMEM((2, 4, 128), f32),
            pltpu.VMEM((2, 2, 4, 128), f32),
            pltpu.SemaphoreType.DMA((4,)),
            pltpu.SemaphoreType.DMA((19,)),
            pltpu.SemaphoreType.DMA((19,)),
            pltpu.SemaphoreType.REGULAR,
            pltpu.SemaphoreType.REGULAR,
            pltpu.SemaphoreType.REGULAR,
            pltpu.SemaphoreType.REGULAR,
            pltpu.SemaphoreType.REGULAR,
        ],
        name="section",
        compiler_params=pltpu.CompilerParams(collective_id=0, has_side_effects=True),
    )(cells, faces)
    return pl.pallas_call(
        write_out,
        out_shape=tuple(jax.ShapeDtypeStruct(shape, f32) for shape in shapes),
        in_specs=[pl.BlockSpec(memory_space=pltpu.VMEM)] * 2,
        out_specs=(pl.BlockSpec(memory_space=pl.ANY),) * 2,
        scratch_shapes=[pltpu.SemaphoreType.DMA((2,))],
        name="write_out",
    )(*(pltpu.with_memory_space_constraint(x, pltpu.VMEM) for x in outputs))


def solution(mesh):
    spec = P(None, "row", "th", "ph")
    return jax.shard_map(on_device, mesh=mesh, in_specs=(spec, spec), out_specs=(spec, spec), check_vma=False)
```

```python
import jax
import jax.numpy as jnp
from jax import lax
from jax.experimental import pallas as pl
from jax.experimental.pallas import tpu as pltpu
from jax.sharding import PartitionSpec as P

MESH = pl.DeviceIdType.MESH
STEP = 0.05
QUARTER = 0.0125
GAMMA = 5.0 / 3.0

ROW_UP, ROW_DOWN, FACE_R, PACK_UP, PACK_DOWN, TH_UP, TH_DOWN, FACE_T = range(8)
CORNER_UP, CORNER_DOWN, PAIR_UP, PAIR_DOWN, LOW_UP, LOW_DOWN, HIGH_UP, HIGH_DOWN = range(8, 16)
E1_UP, E1_DOWN, DIRECT = 16, 17, 18

LEAVE = (
    ((ROW_UP, PAIR_UP), 144),
    ((ROW_DOWN, FACE_R, PAIR_DOWN), 160),
    ((TH_UP, CORNER_UP, E1_UP), 38),
    ((TH_DOWN, FACE_T, CORNER_DOWN, E1_DOWN), 42),
    ((PACK_UP, PACK_DOWN, LOW_UP, LOW_DOWN, HIGH_DOWN), 28),
    ((HIGH_UP,), 4),
    ((DIRECT,), 4),
)
ARRIVE = (
    ((ROW_UP,), 128),
    ((ROW_DOWN, FACE_R), 144),
    ((PACK_UP, PACK_DOWN), 16),
    ((TH_UP, CORNER_UP), 34),
    ((TH_DOWN, FACE_T, CORNER_DOWN), 38),
    ((PAIR_UP,), 16),
    ((PAIR_DOWN,), 16),
    ((LOW_UP, HIGH_UP), 8),
    ((LOW_DOWN, HIGH_DOWN), 8),
    ((E1_UP,), 4),
    ((E1_DOWN,), 4),
)


def group_of(groups, kind):
    return next(i for i, (kinds, _) in enumerate(groups) if kind in kinds)


def cell_state(w):
    density, v0, v1, v2, pressure, b0, b1, b2 = w
    kinetic = 0.5 * density * (v0 * v0 + v1 * v1 + v2 * v2)
    magnetic_sq = b0 * b0 + b1 * b1 + b2 * b2
    energy = pressure / (GAMMA - 1.0) + kinetic + 0.5 * magnetic_sq
    conserved = [density, density * v0, density * v1, density * v2, energy]
    return conserved, magnetic_sq


def flux(w, conserved, magnetic_sq, direction):
    density, v0, v1, v2, pressure, b0, b1, b2 = w
    velocity = (v0, v1, v2)
    magnetic = (b0, b1, b2)
    moving = velocity[direction]
    normal = magnetic[direction]
    total_press = pressure + 0.5 * magnetic_sq
    alignment = v0 * b0 + v1 * b1 + v2 * b2
    fast = jnp.sqrt((GAMMA * pressure + magnetic_sq) / density)
    out = [conserved[direction + 1]]
    for component in range(3):
        moment = conserved[component + 1] * moving - magnetic[component] * normal
        if component == direction:
            moment = moment + total_press
        out.append(moment)
    out.append((conserved[4] + total_press) * moving - normal * alignment)
    return out, jnp.abs(moving) + fast


def quantities(w, direction):
    conserved, magnetic_sq = cell_state(w)
    fluxes, speed = flux(w, conserved, magnetic_sq, direction)
    return conserved, fluxes, speed


def face_flux(lower, upper):
    u_low, f_low, s_low = lower
    u_up, f_up, s_up = upper
    half = 0.5 * jnp.maximum(s_low, s_up)
    return [0.5 * (f_low[i] + f_up[i]) - half * (u_up[i] - u_low[i]) for i in range(5)]


def emf(w, component):
    a, b = ((2, 3), (3, 1), (1, 2))[component]
    return -(w[a] * w[b + 4] - w[b] * w[a + 4])


def kernel(
    cells_hbm, faces_hbm, state, faces_new,
    cv, fv, first_rows, rlo, rhi, f0hi, packs, gp, th_src, gt, f1_src, f1hi, cr_src, cr, pr, e1_corner, e1_src, e1g, e1f, tokens,
    load_sem, send_sem, recv_sem, ok_near, ok_wrap, ok_th,
):
    row = lax.axis_index("row")
    th = lax.axis_index("th")
    ph = lax.axis_index("ph")
    rows, ths, phs = lax.axis_size("row"), lax.axis_size("th"), lax.axis_size("ph")
    z = th * phs + ph
    depth = ths * phs
    at_bottom, at_top = row == 0, row == rows - 1
    at_north, at_south = th == 0, th == ths - 1
    first_z = z == 0
    corner_place = z == 2 * phs - 1
    beside_corner = z == 2 * phs - 2
    corner_sender = (corner_place & (row > 0)) | ((z == phs) & (row == 0))

    def place(dr=0, dt=0, dp=0):
        return {"row": row + dr, "th": th + dt, "ph": lax.rem(ph + dp + phs, phs)}

    load_cells = pltpu.make_async_copy(cells_hbm, cv, load_sem.at[0])
    load_faces = pltpu.make_async_copy(faces_hbm, fv, load_sem.at[1])
    load_velocity = pltpu.make_async_copy(cells_hbm.at[2:4, :, 0:8], first_rows.at[0:2], load_sem.at[2])
    load_field = pltpu.make_async_copy(cells_hbm.at[6:8, :, 0:8], first_rows.at[2:4], load_sem.at[2])

    @pl.when(corner_sender)
    def _():
        load_velocity.start()
        load_field.start()

    load_cells.start()
    load_faces.start()

    barrier = pltpu.get_barrier_semaphore()

    def tell(semaphore, condition, target):
        @pl.when(condition)
        def _():
            pl.semaphore_signal(semaphore, inc=1, device_id=target, device_id_type=MESH)

    def told(semaphore, condition):
        @pl.when(condition)
        def _():
            pl.semaphore_wait(semaphore, 1)

    has_up, has_down = th < ths - 1, th > 0
    first_p, last_p = ph == 0, ph == phs - 1
    inner_up, inner_down = ph < phs - 1, ph > 0
    row_up, row_down = row < rows - 1, row > 0
    plain = jnp.logical_not(corner_place)
    tell(barrier, row_up & plain, place(dr=1))
    tell(barrier, row_down & plain, place(dr=-1))
    tell(barrier, corner_place, place(dp=-1))
    tell(barrier, inner_up, place(dp=1))
    tell(barrier, has_up, place(dt=1))
    tell(barrier, first_p, place(dp=-1))
    tell(barrier, (z == 0) & (row > 0), {"row": row, "th": 1, "ph": phs - 1})
    tell(barrier, (z == 1) & (row == 0), {"row": row, "th": 1, "ph": 0})

    def copy(kind, src, dst, target, recv=None):
        return pltpu.make_async_remote_copy(
            src_ref=src, dst_ref=dst, send_sem=send_sem.at[group_of(LEAVE, kind)],
            recv_sem=recv_sem.at[group_of(ARRIVE, kind if recv is None else recv)],
            device_id=target, device_id_type=MESH,
        )

    up_r, down_r = place(dr=1), place(dr=-1)
    up_t, down_t = place(dt=1), place(dt=-1)
    up_p, down_p = place(dp=1), place(dp=-1)
    origin = {"row": row, "th": th * 0, "ph": (row == 0).astype(jnp.int32)}
    copies = {
        ROW_UP: copy(ROW_UP, cv.at[:, 3], rlo, up_r),
        ROW_DOWN: copy(ROW_DOWN, cv.at[:, 0], rhi, down_r),
        FACE_R: copy(FACE_R, fv.at[0, 0], f0hi, down_r),
        PACK_UP: copy(PACK_UP, packs.at[1], gp.at[0], up_p),
        PACK_DOWN: copy(PACK_DOWN, packs.at[0], gp.at[1], down_p),
        TH_UP: copy(TH_UP, th_src.at[1], gt.at[0], up_t),
        TH_DOWN: copy(TH_DOWN, th_src.at[0], gt.at[1], down_t),
        FACE_T: copy(FACE_T, f1_src, f1hi, down_t),
        CORNER_UP: copy(CORNER_UP, cr_src.at[1], cr.at[0], up_t),
        CORNER_DOWN: copy(CORNER_DOWN, cr_src.at[0], cr.at[1], down_t),
        PAIR_UP: copy(PAIR_UP, gp, pr.at[0], up_r),
        PAIR_DOWN: copy(PAIR_DOWN, gp, pr.at[1], down_r),
        E1_UP: copy(E1_UP, e1_src.at[1], e1g.at[0], up_t),
        E1_DOWN: copy(E1_DOWN, e1_src.at[0], e1g.at[1], down_t),
        LOW_UP: copy(LOW_UP, e1g.at[0], e1f.at[0, 0], up_p),
        LOW_DOWN: copy(LOW_DOWN, e1g.at[0], e1f.at[1, 0], down_p),
        HIGH_UP: copy(HIGH_UP, e1g.at[1], e1f.at[0, 1], up_p),
        HIGH_DOWN: copy(HIGH_DOWN, e1g.at[1], e1f.at[1, 1], down_p),
    }
    direct_left = copy(DIRECT, e1_corner, e1f.at[0, 1], origin, HIGH_UP)

    def send(kind, condition=None):
        if condition is None:
            copies[kind].start()
        else:
            pl.when(condition)(copies[kind].start)

    def all_of(groups, semaphores, kind, condition):
        group = group_of(groups, kind)
        part = tokens.at[0 : groups[group][1]]
        wait = pltpu.make_async_copy(part, part, semaphores.at[group]).wait
        if condition is None:
            wait()
        else:
            pl.when(condition)(wait)

    def arrived(kind, condition=None):
        all_of(ARRIVE, recv_sem, kind, condition)

    def left_here(kind, condition=None):
        all_of(LEAVE, send_sem, kind, condition)

    @pl.when(corner_sender)
    def _():
        pltpu.make_async_copy(first_rows, first_rows, load_sem.at[2]).wait()
        for r in range(4):
            w = [first_rows[k, r, 0:1] for k in range(4)]
            e1_corner[r : r + 1] = -(w[0] * w[3] - w[1] * w[2])

    def number(*conditions):
        total = jnp.int32(0)
        for condition in conditions:
            total = total + condition.astype(jnp.int32)
        return total

    pl.semaphore_wait(
        barrier,
        number(corner_sender, has_down, last_p, row_down & plain, row_up & plain, inner_down, beside_corner),
    )
    pl.when(corner_sender)(direct_left.start)
    tell(ok_th, has_down, place(dt=-1))
    tell(ok_wrap, last_p, place(dp=1))
    tell(ok_near, inner_down & plain, place(dp=-1))
    tell(ok_near, beside_corner & row_up, place(dr=1))
    tell(ok_near, beside_corner & row_down, place(dr=-1))

    load_cells.wait()
    send(ROW_UP, row_up & plain)
    send(ROW_DOWN, row_down & plain)
    for r in range(4):
        for f in range(8):
            th_src[0, f * 4 + r : f * 4 + r + 1] = cv[f, r, 0:1]
            th_src[1, f * 4 + r : f * 4 + r + 1] = cv[f, r, 15:16]
    for side in range(2):
        e1_src[side] = emf([th_src[side, f * 4 : f * 4 + 4] for f in range(8)], 0)
    send(E1_DOWN, has_down)
    load_faces.wait()
    send(FACE_R, row_down & plain)
    for r in range(4):
        f1_src[r : r + 1] = fv[1, r, 0:1]
    third = fv[2].reshape(64, 128)
    turned = jnp.concatenate([third, third], axis=0).T
    for c in range(4, 8):
        packs[0, c : c + 1] = turned[0:1]
        packs[1, c : c + 1] = turned[127:128]
    send(TH_DOWN, has_down)
    send(FACE_T, has_down)
    for c in range(4):
        turned = cv[2 * c : 2 * c + 2].reshape(128, 128).T
        packs[0, c : c + 1] = turned[0:1]
        packs[1, c : c + 1] = turned[127:128]

    @pl.when(at_bottom)
    def _():
        rlo[...] = cv[:, 0]

    @pl.when(at_top)
    def _():
        rhi[...] = cv[:, 3]
        f0hi[...] = fv[0, 3]

    def fill_polar(side, condition):
        @pl.when(condition)
        def _():
            for f in range(8):
                rows_f = th_src[side, f * 4 : f * 4 + 4]
                gt[side, f * 4 : f * 4 + 4] = -rows_f if f in (2, 7) else rows_f

    fill_polar(0, at_north)
    fill_polar(1, at_south)

    def ghost_rows(side):
        return [gt[side, f * 4 : f * 4 + 4] for f in range(8)]

    @pl.when(at_north)
    def _():
        e1g[0] = emf(ghost_rows(0), 0)

    @pl.when(at_south)
    def _():
        e1g[1] = emf(ghost_rows(1), 0)

    send(PACK_DOWN, inner_down)
    send(PACK_UP, last_p)
    send(LOW_DOWN, at_north & inner_down)
    send(LOW_UP, at_north & last_p)

    @pl.when(beside_corner)
    def _():
        pl.semaphore_wait(ok_near, number(row_up, row_down))

    tell(ok_near, beside_corner, place(dp=1))
    told(ok_near, corner_place)
    send(ROW_UP, row_up & corner_place)
    send(ROW_DOWN, row_down & corner_place)
    send(FACE_R, row_down & corner_place)

    arrived(ROW_UP, row_down)
    arrived(ROW_DOWN, row_up)
    for side, line in ((0, 0), (1, 15)):
        for k, ghost in enumerate((rlo, rhi)):
            w = [ghost[f, line : line + 1] for f in range(8)]
            cr_src[side, k : k + 1] = emf(w, 2)

    def fill_corner(side, line, condition):
        @pl.when(condition)
        def _():
            for k, ghost in enumerate((rlo, rhi)):
                w = [ghost[f, line : line + 1] for f in range(8)]
                w[2] = -w[2]
                cr[side, k : k + 1] = emf(w, 2)

    fill_corner(0, 0, at_north)
    fill_corner(1, 15, at_south)
    send(CORNER_DOWN, has_down)

    told(ok_near, inner_up & jnp.logical_not(beside_corner))
    send(PACK_UP, inner_up)
    send(LOW_UP, at_north & inner_up)

    shape = (4, 16, 128)
    lane = lax.broadcasted_iota(jnp.int32, shape, 2)
    line = lax.broadcasted_iota(jnp.int32, shape, 1)
    own = [cv[f] for f in range(8)]

    def ahead_t(x):
        return pltpu.roll(x, 15, 1)

    def behind_t(x):
        return pltpu.roll(x, 1, 1)

    def ahead_p(x):
        return pltpu.roll(x, 127, 2)

    def behind_p(x):
        return pltpu.roll(x, 1, 2)

    low = quantities([rlo[f][None] for f in range(8)], 0)
    mid = quantities(own, 0)
    high = quantities([rhi[f][None] for f in range(8)], 0)

    def tall(a, b, c):
        return jnp.concatenate([a, b, c], axis=0)

    u6 = [tall(low[0][i], mid[0][i], high[0][i]) for i in range(5)]
    g6 = [tall(low[1][i], mid[1][i], high[1][i]) for i in range(5)]
    s6 = tall(low[2], mid[2], high[2])
    face = face_flux(([u[:-1] for u in u6], [g[:-1] for g in g6], s6[:-1]), ([u[1:] for u in u6], [g[1:] for g in g6], s6[1:]))
    for i in range(5):
        state[i] = mid[0][i] - STEP * (face[i][1:] - face[i][:-1])

    told(ok_wrap, first_p)
    send(PACK_DOWN, first_p)
    send(LOW_DOWN, at_north & first_p)

    def send_up(condition):
        told(ok_th, condition)
        send(E1_UP, condition)

    send_up(has_up & last_p)

    arrived(PACK_UP)
    send(PAIR_UP, row_up)
    send(PAIR_DOWN, row_down)
    columns = jnp.concatenate([gp[0], gp[1]], axis=0).T

    def column(side, c, half):
        col = columns[half * 64 : half * 64 + 64, side * 8 + c : side * 8 + c + 1]
        return jnp.broadcast_to(col, (64, 128)).reshape(shape)

    left, right = lane == 0, lane == 127
    beside = [
        jnp.where(left, column(0, f // 2, f % 2), jnp.where(right, column(1, f // 2, f % 2), own[f]))
        for f in range(8)
    ]
    upper_third = column(1, 4, 0)
    e1_beside, e2_beside = emf(beside, 0), emf(beside, 1)

    def apply(direction, outer, ahead, behind, is_low, is_high):
        mine = quantities(own, direction)
        edge = quantities(outer, direction)

        def shifted(a, b):
            return jnp.where(is_high, b, ahead(a))

        above = (
            [shifted(mine[0][i], edge[0][i]) for i in range(5)],
            [shifted(mine[1][i], edge[1][i]) for i in range(5)],
            shifted(mine[2], edge[2]),
        )
        upper = face_flux(mine, above)
        lower = face_flux(edge, mine)
        for i in range(5):
            below = jnp.where(is_low, lower[i], behind(upper[i]))
            state[i] = state[i] - STEP * (upper[i] - below)

    apply(2, beside, ahead_p, behind_p, left, right)
    send_up(has_up & jnp.logical_not(last_p))

    arrived(E1_UP, has_down)
    send(LOW_UP, has_down)
    send(LOW_DOWN, has_down)
    arrived(E1_DOWN, has_up)
    high_up = jnp.logical_not(((z == phs - 1) & (row > 0)) | ((z == 0) & (row == 0)))
    send(HIGH_UP, high_up)
    send(HIGH_DOWN)
    send(TH_UP, has_up)
    send(CORNER_UP, has_up)

    arrived(TH_UP, has_down)
    arrived(TH_DOWN, has_up)

    north, south = line == 0, line == 15

    def spread(ref, *index):
        return jnp.concatenate([jnp.broadcast_to(ref[index + (slice(start, start + 1),)], (16, 128))[None] for start in spread.rows], axis=0)

    def polar(f):
        spread.rows = [f * 4 + r for r in range(4)]
        return jnp.where(north, spread(gt, 0), jnp.where(south, spread(gt, 1), own[f]))

    outside = [polar(f) for f in range(8)]
    apply(1, outside, ahead_t, behind_t, north, south)
    e1_outside, e3_outside = emf(outside, 0), emf(outside, 2)

    arrived(PAIR_UP, row_down)
    arrived(PAIR_DOWN, row_up)

    def pair_emf(ref, *index):
        rows8 = ref[index] if index else ref[...]
        return -(rows8[1:2] * rows8[2:3] - rows8[0:1] * rows8[3:4])

    pair_rows = [pair_emf(gp, 0), pair_emf(gp, 1), pair_emf(pr, 0, 0), pair_emf(pr, 0, 1), pair_emf(pr, 1, 0), pair_emf(pr, 1, 1)]
    pair_columns = jnp.concatenate(pair_rows + [pair_rows[0], pair_rows[0]], axis=0).T

    def pair_ghost(side):
        lanes = lane[:1]
        parts = []
        for k in range(2):
            near = pair_columns[64:80, k : k + 1] if side == 0 else pair_columns[112:128, k : k + 1]
            far_col = pair_columns[112:128, 2 + k : 3 + k] if side == 0 else pair_columns[64:80, 4 + k : 5 + k]
            edge = at_bottom if side == 0 else at_top
            parts.append(jnp.broadcast_to(jnp.where(edge, near, far_col), (16, 128))[None])
        return jnp.where(lanes == 0, parts[0], parts[1])

    def corner_ghost(k):
        a = jnp.broadcast_to(cr[0, k : k + 1], (16, 128))[None]
        b = jnp.broadcast_to(cr[1, k : k + 1], (16, 128))[None]
        return jnp.where(line[:1] == 0, a, b)

    low_w = [rlo[f][None] for f in range(8)]
    high_w = [rhi[f][None] for f in range(8)]
    e1 = emf(own, 0)
    e2 = tall(emf(low_w, 1), emf(own, 1), emf(high_w, 1))
    e3 = tall(emf(low_w, 2), emf(own, 2), emf(high_w, 2))
    e2_side = tall(pair_ghost(0), e2_beside, pair_ghost(1))
    e3_side = tall(corner_ghost(0), e3_outside, corner_ghost(1))

    six = (6, 16, 128)
    lane6 = lax.broadcasted_iota(jnp.int32, six, 2)
    line6 = lax.broadcasted_iota(jnp.int32, six, 1)
    across_t = jnp.where(line6 == 15, e3_side, ahead_t(e3)) - jnp.where(line6 == 0, e3_side, behind_t(e3))
    across_p = jnp.where(lane6 == 127, e2_side, ahead_p(e2)) - jnp.where(lane6 == 0, e2_side, behind_p(e2))
    curl = across_t - across_p
    new_first = fv[0] - QUARTER * (curl[:4] + curl[1:5])
    new_last = f0hi[...] - QUARTER * (curl[4] + curl[5])
    faces_new[0] = new_first
    last = jnp.where(at_top, new_first[3], new_last)
    state[5] = 0.5 * (new_first + jnp.concatenate([new_first[1:], last[None]], axis=0))

    zero = jnp.zeros(shape, jnp.float32)
    curl = (e2[2:] - e2[:-2]) - (
        jnp.where(south, e1_outside, ahead_t(e1)) - jnp.where(north, e1_outside, behind_t(e1))
    )
    curl_beside = (e2_side[2:] - e2_side[:-2]) - (
        jnp.where(south, zero, ahead_t(e1_beside)) - jnp.where(north, zero, behind_t(e1_beside))
    )
    new_third = fv[2] - QUARTER * (curl + jnp.where(left, curl_beside, behind_p(curl)))
    new_upper = upper_third - QUARTER * (curl + curl_beside)
    faces_new[2] = new_third
    state[7] = 0.5 * (new_third + jnp.where(right, new_upper, ahead_p(new_third)))

    curl = (
        jnp.where(right, e1_beside, ahead_p(e1)) - jnp.where(left, e1_beside, behind_p(e1))
    ) - (e3[2:] - e3[:-2])
    curl_outside = (
        jnp.where(right, zero, ahead_p(e1_outside)) - jnp.where(left, zero, behind_p(e1_outside))
    ) - (e3_side[2:] - e3_side[:-2])
    new_second = fv[1] - QUARTER * (curl + jnp.where(north, curl_outside, behind_t(curl)))
    spread.rows = [0, 1, 2, 3]
    new_upper = spread(f1hi) - QUARTER * (curl + curl_outside)
    new_upper = jnp.where(at_south, 0.0, new_upper)
    faces_new[1] = new_second
    state[6] = 0.5 * (new_second + jnp.where(south, new_upper, ahead_t(new_second)))

    left_here(ROW_UP, row_up)
    left_here(ROW_DOWN, row_down)
    left_here(TH_UP, has_up)
    left_here(TH_DOWN, has_down)
    left_here(PACK_UP)
    left_here(HIGH_UP, high_up)
    left_here(DIRECT, corner_sender)

    lane4 = lax.broadcasted_iota(jnp.int32, (4, 128), 1)

    def from_left(k):
        return QUARTER * jnp.where(lane4 == 0, pltpu.roll(e1f[0, k], 1, 1), 0.0)

    def from_right(k):
        return QUARTER * jnp.where(lane4 == 127, pltpu.roll(e1f[1, k], 127, 1), 0.0)

    keep = jnp.where(at_south, 0.0, 0.5)

    def adjust(ref, r, place_row, amount):
        ref[r, place_row : place_row + 1] = ref[r, place_row : place_row + 1] + amount

    arrived(LOW_DOWN)
    b_low, b_high = from_right(0), from_right(1)
    for r in range(4):
        b = b_low[r : r + 1]
        adjust(faces_new.at[1], r, 0, -b)
        adjust(state.at[6], r, 0, -0.5 * b)
        adjust(state.at[7], r, 0, -0.5 * b)
        b = b_high[r : r + 1]
        adjust(state.at[6], r, 15, -keep * b)
        adjust(state.at[7], r, 15, 0.5 * b)
    arrived(LOW_UP)
    a_low, a_high = from_left(0), from_left(1)
    for r in range(4):
        a = a_low[r : r + 1]
        adjust(faces_new.at[1], r, 0, a)
        adjust(state.at[6], r, 0, 0.5 * a)
        adjust(faces_new.at[2], r, 0, -a)
        adjust(state.at[7], r, 0, -0.5 * a)
        a = a_high[r : r + 1]
        adjust(state.at[6], r, 15, keep * a)
        adjust(faces_new.at[2], r, 15, a)
        adjust(state.at[7], r, 15, 0.5 * a)


def write_out(state, faces_new, state_hbm, faces_hbm, sem):
    copies = [
        pltpu.make_async_copy(state, state_hbm, sem.at[0]),
        pltpu.make_async_copy(faces_new, faces_hbm, sem.at[1]),
    ]
    for copy in copies:
        copy.start()
    for copy in copies:
        copy.wait()


def on_device(cells, faces):
    f32 = jnp.float32
    shapes = ((8, 4, 16, 128), (3, 4, 16, 128))
    outputs = pl.pallas_call(
        kernel,
        out_shape=tuple(pltpu.VMEM(shape, f32) for shape in shapes),
        in_specs=[pl.BlockSpec(memory_space=pl.ANY)] * 2,
        out_specs=(pl.BlockSpec(memory_space=pltpu.VMEM),) * 2,
        scratch_shapes=[
            pltpu.VMEM((8, 4, 16, 128), f32),
            pltpu.VMEM((3, 4, 16, 128), f32),
            pltpu.VMEM((4, 4, 8, 128), f32),
            pltpu.VMEM((8, 16, 128), f32),
            pltpu.VMEM((8, 16, 128), f32),
            pltpu.VMEM((16, 128), f32),
            pltpu.VMEM((2, 8, 128), f32),
            pltpu.VMEM((2, 8, 128), f32),
            pltpu.VMEM((2, 32, 128), f32),
            pltpu.VMEM((2, 32, 128), f32),
            pltpu.VMEM((4, 128), f32),
            pltpu.VMEM((4, 128), f32),
            pltpu.VMEM((2, 2, 128), f32),
            pltpu.VMEM((2, 2, 128), f32),
            pltpu.VMEM((2, 2, 8, 128), f32),
            pltpu.VMEM((4, 128), f32),
            pltpu.VMEM((2, 4, 128), f32),
            pltpu.VMEM((2, 4, 128), f32),
            pltpu.VMEM((2, 2, 4, 128), f32),
            pltpu.VMEM((160, 1, 128), f32),
            pltpu.SemaphoreType.DMA((3,)),
            pltpu.SemaphoreType.DMA((len(LEAVE),)),
            pltpu.SemaphoreType.DMA((len(ARRIVE),)),
            pltpu.SemaphoreType.REGULAR,
            pltpu.SemaphoreType.REGULAR,
            pltpu.SemaphoreType.REGULAR,
        ],
        name="section",
        compiler_params=pltpu.CompilerParams(collective_id=0, has_side_effects=True),
    )(cells, faces)
    return pl.pallas_call(
        write_out,
        out_shape=tuple(jax.ShapeDtypeStruct(shape, f32) for shape in shapes),
        in_specs=[pl.BlockSpec(memory_space=pltpu.VMEM)] * 2,
        out_specs=(pl.BlockSpec(memory_space=pl.ANY),) * 2,
        scratch_shapes=[pltpu.SemaphoreType.DMA((2,))],
        name="write_out",
    )(*(pltpu.with_memory_space_constraint(x, pltpu.VMEM) for x in outputs))


def solution(mesh):
    spec = P(None, "row", "th", "ph")
    return jax.shard_map(on_device, mesh=mesh, in_specs=(spec, spec), out_specs=(spec, spec), check_vma=False)
```

```python
import jax
import jax.numpy as jnp
from jax import lax
from jax.experimental import pallas as pl
from jax.experimental.pallas import tpu as pltpu
from jax.sharding import PartitionSpec as P

MESH = pl.DeviceIdType.MESH
STEP = 0.05
QUARTER = 0.0125
GAMMA = 5.0 / 3.0

ROW_UP, ROW_DOWN, FACE_R, PACK_UP, PACK_DOWN, TH_UP, TH_DOWN, FACE_T = range(8)
CORNER_UP, CORNER_DOWN, PAIR_UP, PAIR_DOWN, LOW_UP, LOW_DOWN, HIGH_UP, HIGH_DOWN = range(8, 16)
E1_UP, E1_DOWN, DIRECT = 16, 17, 18

EDGE = 19

LEAVE = (
    (ROW_UP, PAIR_UP, ROW_DOWN, FACE_R, PAIR_DOWN),
    (TH_UP, CORNER_UP, E1_UP, TH_DOWN, FACE_T, CORNER_DOWN, E1_DOWN),
    (PACK_UP, PACK_DOWN, LOW_UP, LOW_DOWN, HIGH_UP, HIGH_DOWN, DIRECT, EDGE),
)
ARRIVE = (
    (ROW_UP, ROW_DOWN, FACE_R),
    (PACK_UP, PACK_DOWN),
    (TH_UP, CORNER_UP, TH_DOWN, FACE_T, CORNER_DOWN),
    (PAIR_UP, PAIR_DOWN),
    (LOW_UP, HIGH_UP),
    (LOW_DOWN, HIGH_DOWN),
    (E1_UP,),
    (E1_DOWN,),
)


def group_of(groups, kind):
    return next(i for i, kinds in enumerate(groups) if kind in kinds)


def cell_state(w):
    density, v0, v1, v2, pressure, b0, b1, b2 = w
    kinetic = 0.5 * density * (v0 * v0 + v1 * v1 + v2 * v2)
    magnetic_sq = b0 * b0 + b1 * b1 + b2 * b2
    energy = pressure / (GAMMA - 1.0) + kinetic + 0.5 * magnetic_sq
    conserved = [density, density * v0, density * v1, density * v2, energy]
    return conserved, magnetic_sq


def flux(w, conserved, magnetic_sq, direction):
    density, v0, v1, v2, pressure, b0, b1, b2 = w
    velocity = (v0, v1, v2)
    magnetic = (b0, b1, b2)
    moving = velocity[direction]
    normal = magnetic[direction]
    total_press = pressure + 0.5 * magnetic_sq
    alignment = v0 * b0 + v1 * b1 + v2 * b2
    fast = jnp.sqrt((GAMMA * pressure + magnetic_sq) / density)
    out = [conserved[direction + 1]]
    for component in range(3):
        moment = conserved[component + 1] * moving - magnetic[component] * normal
        if component == direction:
            moment = moment + total_press
        out.append(moment)
    out.append((conserved[4] + total_press) * moving - normal * alignment)
    return out, jnp.abs(moving) + fast


def quantities(w, direction):
    conserved, magnetic_sq = cell_state(w)
    fluxes, speed = flux(w, conserved, magnetic_sq, direction)
    return conserved, fluxes, speed


def face_flux(lower, upper):
    u_low, f_low, s_low = lower
    u_up, f_up, s_up = upper
    half = 0.5 * jnp.maximum(s_low, s_up)
    return [0.5 * (f_low[i] + f_up[i]) - half * (u_up[i] - u_low[i]) for i in range(5)]


def emf(w, component):
    a, b = ((2, 3), (3, 1), (1, 2))[component]
    return -(w[a] * w[b + 4] - w[b] * w[a + 4])


def kernel(
    cells_hbm, faces_hbm, state, faces_new,
    cv, fv, first_rows, rlo, rhi, f0hi, packs, gp, th_src, gt, f1_src, f1hi, cr_src, cr, pr, e1_corner, e1_src, e1g, e1f, tokens,
    load_sem, send_sem, recv_sem, ok_near, ok_wrap, ok_th,
):
    row = lax.axis_index("row")
    th = lax.axis_index("th")
    ph = lax.axis_index("ph")
    rows, ths, phs = lax.axis_size("row"), lax.axis_size("th"), lax.axis_size("ph")
    z = th * phs + ph
    depth = ths * phs
    at_bottom, at_top = row == 0, row == rows - 1
    at_north, at_south = th == 0, th == ths - 1
    first_z = z == 0
    corner_place = z == 2 * phs - 1
    beside_corner = z == 2 * phs - 2
    corner_sender = (corner_place & (row > 0)) | ((z == phs) & (row == 0))

    def place(dr=0, dt=0, dp=0):
        return {"row": row + dr, "th": th + dt, "ph": lax.rem(ph + dp + phs, phs)}

    load_cells = pltpu.make_async_copy(cells_hbm, cv, load_sem.at[0])
    load_faces = pltpu.make_async_copy(faces_hbm, fv, load_sem.at[0])
    load_velocity = pltpu.make_async_copy(cells_hbm.at[2:4, :, 0:8], first_rows.at[0:2], load_sem.at[1])
    load_field = pltpu.make_async_copy(cells_hbm.at[6:8, :, 0:8], first_rows.at[2:4], load_sem.at[1])

    @pl.when(corner_sender)
    def _():
        load_velocity.start()
        load_field.start()

    load_cells.start()
    load_faces.start()

    barrier = pltpu.get_barrier_semaphore()

    def tell(semaphore, condition, target):
        @pl.when(condition)
        def _():
            pl.semaphore_signal(semaphore, inc=1, device_id=target, device_id_type=MESH)

    def told(semaphore, condition):
        @pl.when(condition)
        def _():
            pl.semaphore_wait(semaphore, 1)

    has_up, has_down = th < ths - 1, th > 0
    first_p, last_p = ph == 0, ph == phs - 1
    inner_up, inner_down = ph < phs - 1, ph > 0
    row_up, row_down = row < rows - 1, row > 0
    plain = jnp.logical_not(corner_place)
    tell(barrier, row_up & plain, place(dr=1))
    tell(barrier, row_down & plain, place(dr=-1))
    tell(barrier, corner_place, place(dp=-1))
    edge = last_p & has_up
    before_edge = first_p & has_down
    twin_below = (th == ths - 2) & inner_up
    twin_above = at_south & inner_up
    past_edge = {"row": row, "th": th + 1, "ph": ph * 0}
    tell(barrier, twin_above, place(dt=-1))
    tell(barrier, edge, past_edge)
    tell(barrier, inner_up, place(dp=1))
    tell(barrier, has_up, place(dt=1))
    tell(barrier, first_p, place(dp=-1))
    tell(barrier, (z == 0) & (row > 0), {"row": row, "th": 1, "ph": phs - 1})
    tell(barrier, (z == 1) & (row == 0), {"row": row, "th": 1, "ph": 0})

    def copy(kind, src, dst, target, recv=None):
        return pltpu.make_async_remote_copy(
            src_ref=src, dst_ref=dst, send_sem=send_sem.at[group_of(LEAVE, kind)],
            recv_sem=recv_sem.at[group_of(ARRIVE, kind if recv is None else recv)],
            device_id=target, device_id_type=MESH,
        )

    up_r, down_r = place(dr=1), place(dr=-1)
    up_t, down_t = place(dt=1), place(dt=-1)
    up_p, down_p = place(dp=1), place(dp=-1)
    origin = {"row": row, "th": th * 0, "ph": (row == 0).astype(jnp.int32)}
    copies = {
        ROW_UP: copy(ROW_UP, cv.at[:, 3], rlo, up_r),
        ROW_DOWN: copy(ROW_DOWN, cv.at[:, 0], rhi, down_r),
        FACE_R: copy(FACE_R, fv.at[0, 0], f0hi, down_r),
        PACK_UP: copy(PACK_UP, packs.at[1], gp.at[0], up_p),
        PACK_DOWN: copy(PACK_DOWN, packs.at[0], gp.at[1], down_p),
        TH_UP: copy(TH_UP, th_src.at[1], gt.at[0], up_t),
        TH_DOWN: copy(TH_DOWN, th_src.at[0], gt.at[1], down_t),
        FACE_T: copy(FACE_T, f1_src, f1hi, down_t),
        CORNER_UP: copy(CORNER_UP, cr_src.at[1], cr.at[0], up_t),
        CORNER_DOWN: copy(CORNER_DOWN, cr_src.at[0], cr.at[1], down_t),
        PAIR_UP: copy(PAIR_UP, gp, pr.at[0], up_r),
        PAIR_DOWN: copy(PAIR_DOWN, gp, pr.at[1], down_r),
        E1_UP: copy(E1_UP, e1_src.at[1], e1g.at[0], up_t),
        E1_DOWN: copy(E1_DOWN, e1_src.at[0], e1g.at[1], down_t),
        LOW_UP: copy(LOW_UP, e1g.at[0], e1f.at[0, 0], up_p),
        LOW_DOWN: copy(LOW_DOWN, e1g.at[0], e1f.at[1, 0], down_p),
        HIGH_UP: copy(HIGH_UP, e1g.at[1], e1f.at[0, 1], up_p),
        HIGH_DOWN: copy(HIGH_DOWN, e1g.at[1], e1f.at[1, 1], down_p),
    }
    edge_up = copy(EDGE, e1_src.at[1], e1f.at[0, 0], past_edge, LOW_UP)
    direct_left = copy(DIRECT, e1_corner, e1f.at[0, 1], origin, HIGH_UP)

    def send(kind, condition=None):
        if condition is None:
            copies[kind].start()
        else:
            pl.when(condition)(copies[kind].start)

    def take(semaphore, size, condition=None):
        part = tokens.at[0:size]
        wait = pltpu.make_async_copy(part, part, semaphore).wait
        if condition is None:
            wait()
        else:
            pl.when(condition)(wait)

    def take_sides(semaphore, first, first_size, second, second_size):
        take(semaphore, first_size + second_size, first & second)
        take(semaphore, first_size, first & jnp.logical_not(second))
        take(semaphore, second_size, second & jnp.logical_not(first))

    def arrived(kind):
        return recv_sem.at[group_of(ARRIVE, kind)]

    def leaving(kind):
        return send_sem.at[group_of(LEAVE, kind)]

    @pl.when(corner_sender)
    def _():
        pltpu.make_async_copy(first_rows, first_rows, load_sem.at[1]).wait()
        for r in range(4):
            w = [first_rows[k, r, 0:1] for k in range(4)]
            e1_corner[r : r + 1] = -(w[0] * w[3] - w[1] * w[2])

    def number(*conditions):
        total = jnp.int32(0)
        for condition in conditions:
            total = total + condition.astype(jnp.int32)
        return total

    pl.semaphore_wait(
        barrier,
        number(corner_sender, has_down, last_p, row_down & plain, row_up & plain, inner_down, beside_corner)
        + number(before_edge, twin_below),
    )
    pl.when(corner_sender)(direct_left.start)
    tell(ok_th, has_down & jnp.logical_not(twin_above), place(dt=-1))
    tell(ok_wrap, before_edge, {"row": row, "th": th - 1, "ph": ph * 0 + phs - 1})
    tell(ok_wrap, last_p, place(dp=1))
    tell(ok_near, inner_down & plain, place(dp=-1))
    tell(ok_near, beside_corner & row_up, place(dr=1))
    tell(ok_near, beside_corner & row_down, place(dr=-1))

    take(load_sem.at[0], 704)
    send(ROW_UP, row_up & plain)
    send(ROW_DOWN, row_down & plain)
    for r in range(4):
        for f in range(8):
            th_src[0, f * 4 + r : f * 4 + r + 1] = cv[f, r, 0:1]
            th_src[1, f * 4 + r : f * 4 + r + 1] = cv[f, r, 15:16]
    for side in range(2):
        e1_src[side] = emf([th_src[side, f * 4 : f * 4 + 4] for f in range(8)], 0)
    send(E1_DOWN, has_down)
    send(E1_UP, twin_below)
    send(FACE_R, row_down & plain)
    for r in range(4):
        f1_src[r : r + 1] = fv[1, r, 0:1]
    third = fv[2].reshape(64, 128)
    turned = jnp.concatenate([third, third], axis=0).T
    for c in range(4, 8):
        packs[0, c : c + 1] = turned[0:1]
        packs[1, c : c + 1] = turned[127:128]
    send(TH_DOWN, has_down)
    send(FACE_T, has_down)
    send(TH_UP, twin_below)
    for c in range(4):
        turned = cv[2 * c : 2 * c + 2].reshape(128, 128).T
        packs[0, c : c + 1] = turned[0:1]
        packs[1, c : c + 1] = turned[127:128]

    @pl.when(at_bottom)
    def _():
        rlo[...] = cv[:, 0]

    @pl.when(at_top)
    def _():
        rhi[...] = cv[:, 3]
        f0hi[...] = fv[0, 3]

    def fill_polar(side, condition):
        @pl.when(condition)
        def _():
            for f in range(8):
                rows_f = th_src[side, f * 4 : f * 4 + 4]
                gt[side, f * 4 : f * 4 + 4] = -rows_f if f in (2, 7) else rows_f

    fill_polar(0, at_north)
    fill_polar(1, at_south)

    def ghost_rows(side):
        return [gt[side, f * 4 : f * 4 + 4] for f in range(8)]

    @pl.when(at_north)
    def _():
        e1g[0] = emf(ghost_rows(0), 0)

    @pl.when(at_south)
    def _():
        e1g[1] = emf(ghost_rows(1), 0)

    send(PACK_DOWN, inner_down)
    send(PACK_UP, last_p)
    send(LOW_DOWN, at_north & inner_down)
    send(LOW_UP, at_north & last_p)

    @pl.when(beside_corner)
    def _():
        pl.semaphore_wait(ok_near, number(row_up, row_down))

    tell(ok_near, beside_corner, place(dp=1))
    told(ok_near, corner_place)
    send(ROW_UP, row_up & corner_place)
    send(ROW_DOWN, row_down & corner_place)
    send(FACE_R, row_down & corner_place)

    take_sides(arrived(ROW_UP), row_down, 128, row_up, 144)
    for side, line in ((0, 0), (1, 15)):
        for k, ghost in enumerate((rlo, rhi)):
            w = [ghost[f, line : line + 1] for f in range(8)]
            cr_src[side, k : k + 1] = emf(w, 2)

    def fill_corner(side, line, condition):
        @pl.when(condition)
        def _():
            for k, ghost in enumerate((rlo, rhi)):
                w = [ghost[f, line : line + 1] for f in range(8)]
                w[2] = -w[2]
                cr[side, k : k + 1] = emf(w, 2)

    fill_corner(0, 0, at_north)
    fill_corner(1, 15, at_south)
    send(CORNER_DOWN, has_down)
    send(CORNER_UP, twin_below)

    told(ok_near, inner_up & jnp.logical_not(beside_corner))
    send(PACK_UP, inner_up)
    send(LOW_UP, at_north & inner_up)

    shape = (4, 16, 128)
    lane = lax.broadcasted_iota(jnp.int32, shape, 2)
    line = lax.broadcasted_iota(jnp.int32, shape, 1)
    own = [cv[f] for f in range(8)]

    def ahead_t(x):
        return pltpu.roll(x, 15, 1)

    def behind_t(x):
        return pltpu.roll(x, 1, 1)

    def ahead_p(x):
        return pltpu.roll(x, 127, 2)

    def behind_p(x):
        return pltpu.roll(x, 1, 2)

    low = quantities([rlo[f][None] for f in range(8)], 0)
    mid = quantities(own, 0)
    high = quantities([rhi[f][None] for f in range(8)], 0)

    def tall(a, b, c):
        return jnp.concatenate([a, b, c], axis=0)

    u6 = [tall(low[0][i], mid[0][i], high[0][i]) for i in range(5)]
    g6 = [tall(low[1][i], mid[1][i], high[1][i]) for i in range(5)]
    s6 = tall(low[2], mid[2], high[2])
    face = face_flux(([u[:-1] for u in u6], [g[:-1] for g in g6], s6[:-1]), ([u[1:] for u in u6], [g[1:] for g in g6], s6[1:]))
    for i in range(5):
        state[i] = mid[0][i] - STEP * (face[i][1:] - face[i][:-1])

    told(ok_wrap, first_p | edge)
    pl.when(edge)(edge_up.start)
    send(PACK_DOWN, first_p)
    send(LOW_DOWN, at_north & first_p)

    def send_up(condition):
        told(ok_th, condition)
        send(E1_UP, condition)
        send(TH_UP, condition)
        send(CORNER_UP, condition)

    send_up(has_up & last_p)

    take(arrived(PACK_UP), 16)
    send(PAIR_UP, row_up)
    send(PAIR_DOWN, row_down)
    columns = jnp.concatenate([gp[0], gp[1]], axis=0).T

    def column(side, c, half):
        col = columns[half * 64 : half * 64 + 64, side * 8 + c : side * 8 + c + 1]
        return jnp.broadcast_to(col, (64, 128)).reshape(shape)

    left, right = lane == 0, lane == 127
    beside = [
        jnp.where(left, column(0, f // 2, f % 2), jnp.where(right, column(1, f // 2, f % 2), own[f]))
        for f in range(8)
    ]
    upper_third = column(1, 4, 0)
    e1_beside, e2_beside = emf(beside, 0), emf(beside, 1)

    def apply(direction, outer, ahead, behind, is_low, is_high):
        mine = quantities(own, direction)
        edge = quantities(outer, direction)

        def shifted(a, b):
            return jnp.where(is_high, b, ahead(a))

        above = (
            [shifted(mine[0][i], edge[0][i]) for i in range(5)],
            [shifted(mine[1][i], edge[1][i]) for i in range(5)],
            shifted(mine[2], edge[2]),
        )
        upper = face_flux(mine, above)
        lower = face_flux(edge, mine)
        for i in range(5):
            below = jnp.where(is_low, lower[i], behind(upper[i]))
            state[i] = state[i] - STEP * (upper[i] - below)

    apply(2, beside, ahead_p, behind_p, left, right)
    send_up(has_up & inner_up & jnp.logical_not(twin_below))

    high_up = jnp.logical_not(((z == phs - 1) & (row > 0)) | ((z == 0) & (row == 0)))

    def pass_high(condition):
        take(arrived(E1_DOWN), 4, has_up & condition)
        send(HIGH_UP, high_up & condition)
        send(HIGH_DOWN, condition)

    pass_high(last_p)
    take(arrived(E1_UP), 4, has_down)
    send(LOW_UP, has_down & inner_up)
    send(LOW_DOWN, has_down)
    pass_high(inner_up)

    take_sides(arrived(TH_UP), has_down, 34, has_up, 38)

    north, south = line == 0, line == 15

    def spread(ref, *index):
        return jnp.concatenate([jnp.broadcast_to(ref[index + (slice(start, start + 1),)], (16, 128))[None] for start in spread.rows], axis=0)

    def polar(f):
        spread.rows = [f * 4 + r for r in range(4)]
        return jnp.where(north, spread(gt, 0), jnp.where(south, spread(gt, 1), own[f]))

    outside = [polar(f) for f in range(8)]
    apply(1, outside, ahead_t, behind_t, north, south)
    e1_outside, e3_outside = emf(outside, 0), emf(outside, 2)

    take_sides(arrived(PAIR_UP), row_down, 16, row_up, 16)

    def pair_emf(ref, *index):
        rows8 = ref[index] if index else ref[...]
        return -(rows8[1:2] * rows8[2:3] - rows8[0:1] * rows8[3:4])

    pair_rows = [pair_emf(gp, 0), pair_emf(gp, 1), pair_emf(pr, 0, 0), pair_emf(pr, 0, 1), pair_emf(pr, 1, 0), pair_emf(pr, 1, 1)]
    pair_columns = jnp.concatenate(pair_rows + [pair_rows[0], pair_rows[0]], axis=0).T

    def pair_ghost(side):
        lanes = lane[:1]
        parts = []
        for k in range(2):
            near = pair_columns[64:80, k : k + 1] if side == 0 else pair_columns[112:128, k : k + 1]
            far_col = pair_columns[112:128, 2 + k : 3 + k] if side == 0 else pair_columns[64:80, 4 + k : 5 + k]
            edge = at_bottom if side == 0 else at_top
            parts.append(jnp.broadcast_to(jnp.where(edge, near, far_col), (16, 128))[None])
        return jnp.where(lanes == 0, parts[0], parts[1])

    def corner_ghost(k):
        a = jnp.broadcast_to(cr[0, k : k + 1], (16, 128))[None]
        b = jnp.broadcast_to(cr[1, k : k + 1], (16, 128))[None]
        return jnp.where(line[:1] == 0, a, b)

    low_w = [rlo[f][None] for f in range(8)]
    high_w = [rhi[f][None] for f in range(8)]
    e1 = emf(own, 0)
    e2 = tall(emf(low_w, 1), emf(own, 1), emf(high_w, 1))
    e3 = tall(emf(low_w, 2), emf(own, 2), emf(high_w, 2))
    e2_side = tall(pair_ghost(0), e2_beside, pair_ghost(1))
    e3_side = tall(corner_ghost(0), e3_outside, corner_ghost(1))

    six = (6, 16, 128)
    lane6 = lax.broadcasted_iota(jnp.int32, six, 2)
    line6 = lax.broadcasted_iota(jnp.int32, six, 1)
    across_t = jnp.where(line6 == 15, e3_side, ahead_t(e3)) - jnp.where(line6 == 0, e3_side, behind_t(e3))
    across_p = jnp.where(lane6 == 127, e2_side, ahead_p(e2)) - jnp.where(lane6 == 0, e2_side, behind_p(e2))
    curl = across_t - across_p
    new_first = fv[0] - QUARTER * (curl[:4] + curl[1:5])
    new_last = f0hi[...] - QUARTER * (curl[4] + curl[5])
    faces_new[0] = new_first
    last = jnp.where(at_top, new_first[3], new_last)
    state[5] = 0.5 * (new_first + jnp.concatenate([new_first[1:], last[None]], axis=0))

    zero = jnp.zeros(shape, jnp.float32)
    curl = (e2[2:] - e2[:-2]) - (
        jnp.where(south, e1_outside, ahead_t(e1)) - jnp.where(north, e1_outside, behind_t(e1))
    )
    curl_beside = (e2_side[2:] - e2_side[:-2]) - (
        jnp.where(south, zero, ahead_t(e1_beside)) - jnp.where(north, zero, behind_t(e1_beside))
    )
    new_third = fv[2] - QUARTER * (curl + jnp.where(left, curl_beside, behind_p(curl)))
    new_upper = upper_third - QUARTER * (curl + curl_beside)
    faces_new[2] = new_third
    state[7] = 0.5 * (new_third + jnp.where(right, new_upper, ahead_p(new_third)))

    curl = (
        jnp.where(right, e1_beside, ahead_p(e1)) - jnp.where(left, e1_beside, behind_p(e1))
    ) - (e3[2:] - e3[:-2])
    curl_outside = (
        jnp.where(right, zero, ahead_p(e1_outside)) - jnp.where(left, zero, behind_p(e1_outside))
    ) - (e3_side[2:] - e3_side[:-2])
    new_second = fv[1] - QUARTER * (curl + jnp.where(north, curl_outside, behind_t(curl)))
    spread.rows = [0, 1, 2, 3]
    new_upper = spread(f1hi) - QUARTER * (curl + curl_outside)
    new_upper = jnp.where(at_south, 0.0, new_upper)
    faces_new[1] = new_second
    state[6] = 0.5 * (new_second + jnp.where(south, new_upper, ahead_t(new_second)))

    take_sides(leaving(ROW_UP), row_up, 144, row_down, 160)
    take_sides(leaving(TH_UP), has_up, 38, has_down, 42)
    extra = number(inner_up | at_north, high_up, corner_sender, edge)
    for k in range(5):
        take(leaving(PACK_UP), 24 + 4 * k, extra == k)

    lane4 = lax.broadcasted_iota(jnp.int32, (4, 128), 1)

    def from_left(k):
        return QUARTER * jnp.where(lane4 == 0, pltpu.roll(e1f[0, k], 1, 1), 0.0)

    def from_right(k):
        return QUARTER * jnp.where(lane4 == 127, pltpu.roll(e1f[1, k], 127, 1), 0.0)

    keep = jnp.where(at_south, 0.0, 0.5)

    def adjust(ref, r, place_row, amount):
        ref[r, place_row : place_row + 1] = ref[r, place_row : place_row + 1] + amount

    take(arrived(LOW_DOWN), 8)
    b_low, b_high = from_right(0), from_right(1)
    for r in range(4):
        b = b_low[r : r + 1]
        adjust(faces_new.at[1], r, 0, -b)
        adjust(state.at[6], r, 0, -0.5 * b)
        adjust(state.at[7], r, 0, -0.5 * b)
        b = b_high[r : r + 1]
        adjust(state.at[6], r, 15, -keep * b)
        adjust(state.at[7], r, 15, 0.5 * b)
    take(arrived(LOW_UP), 8)
    a_low, a_high = from_left(0), from_left(1)
    for r in range(4):
        a = a_low[r : r + 1]
        adjust(faces_new.at[1], r, 0, a)
        adjust(state.at[6], r, 0, 0.5 * a)
        adjust(faces_new.at[2], r, 0, -a)
        adjust(state.at[7], r, 0, -0.5 * a)
        a = a_high[r : r + 1]
        adjust(state.at[6], r, 15, keep * a)
        adjust(faces_new.at[2], r, 15, a)
        adjust(state.at[7], r, 15, 0.5 * a)


def write_out(state, faces_new, state_hbm, faces_hbm, sem):
    copies = [
        pltpu.make_async_copy(state, state_hbm, sem.at[0]),
        pltpu.make_async_copy(faces_new, faces_hbm, sem.at[1]),
    ]
    for copy in copies:
        copy.start()
    for copy in copies:
        copy.wait()


def on_device(cells, faces):
    f32 = jnp.float32
    shapes = ((8, 4, 16, 128), (3, 4, 16, 128))
    outputs = pl.pallas_call(
        kernel,
        out_shape=tuple(pltpu.VMEM(shape, f32) for shape in shapes),
        in_specs=[pl.BlockSpec(memory_space=pl.ANY)] * 2,
        out_specs=(pl.BlockSpec(memory_space=pltpu.VMEM),) * 2,
        scratch_shapes=[
            pltpu.VMEM((8, 4, 16, 128), f32),
            pltpu.VMEM((3, 4, 16, 128), f32),
            pltpu.VMEM((4, 4, 8, 128), f32),
            pltpu.VMEM((8, 16, 128), f32),
            pltpu.VMEM((8, 16, 128), f32),
            pltpu.VMEM((16, 128), f32),
            pltpu.VMEM((2, 8, 128), f32),
            pltpu.VMEM((2, 8, 128), f32),
            pltpu.VMEM((2, 32, 128), f32),
            pltpu.VMEM((2, 32, 128), f32),
            pltpu.VMEM((4, 128), f32),
            pltpu.VMEM((4, 128), f32),
            pltpu.VMEM((2, 2, 128), f32),
            pltpu.VMEM((2, 2, 128), f32),
            pltpu.VMEM((2, 2, 8, 128), f32),
            pltpu.VMEM((4, 128), f32),
            pltpu.VMEM((2, 4, 128), f32),
            pltpu.VMEM((2, 4, 128), f32),
            pltpu.VMEM((2, 2, 4, 128), f32),
            pltpu.VMEM((704, 1, 128), f32),
            pltpu.SemaphoreType.DMA((2,)),
            pltpu.SemaphoreType.DMA((len(LEAVE),)),
            pltpu.SemaphoreType.DMA((len(ARRIVE),)),
            pltpu.SemaphoreType.REGULAR,
            pltpu.SemaphoreType.REGULAR,
            pltpu.SemaphoreType.REGULAR,
        ],
        name="section",
        compiler_params=pltpu.CompilerParams(collective_id=0, has_side_effects=True),
    )(cells, faces)
    return pl.pallas_call(
        write_out,
        out_shape=tuple(jax.ShapeDtypeStruct(shape, f32) for shape in shapes),
        in_specs=[pl.BlockSpec(memory_space=pltpu.VMEM)] * 2,
        out_specs=(pl.BlockSpec(memory_space=pl.ANY),) * 2,
        scratch_shapes=[pltpu.SemaphoreType.DMA((2,))],
        name="write_out",
    )(*(pltpu.with_memory_space_constraint(x, pltpu.VMEM) for x in outputs))


def solution(mesh):
    spec = P(None, "row", "th", "ph")
    return jax.shard_map(on_device, mesh=mesh, in_specs=(spec, spec), out_specs=(spec, spec), check_vma=False)
```

```python
import jax
import jax.numpy as jnp
from jax import lax
from jax.experimental import pallas as pl
from jax.experimental.pallas import tpu as pltpu
from jax.sharding import PartitionSpec as P

MESH = pl.DeviceIdType.MESH
STEP = 0.05
QUARTER = 0.0125
GAMMA = 5.0 / 3.0

ROW_UP, ROW_DOWN, FACE_R, PACK_UP, PACK_DOWN, TH_UP, TH_DOWN, FACE_T = range(8)
CORNER_UP, CORNER_DOWN, PAIR_UP, PAIR_DOWN, LOW_UP, LOW_DOWN, HIGH_UP, HIGH_DOWN = range(8, 16)
E1_UP, E1_DOWN, DIRECT = 16, 17, 18

EDGE = 19

LEAVE = (
    (ROW_UP, PAIR_UP, ROW_DOWN, FACE_R, PAIR_DOWN),
    (TH_UP, CORNER_UP, E1_UP, TH_DOWN, FACE_T, CORNER_DOWN, E1_DOWN),
    (PACK_UP, PACK_DOWN, LOW_UP, LOW_DOWN, HIGH_UP, HIGH_DOWN, DIRECT, EDGE),
)
ARRIVE = (
    (ROW_UP, ROW_DOWN, FACE_R),
    (PACK_UP, PACK_DOWN),
    (TH_UP, CORNER_UP, TH_DOWN, FACE_T, CORNER_DOWN),
    (PAIR_UP, PAIR_DOWN),
    (LOW_UP, HIGH_UP),
    (LOW_DOWN, HIGH_DOWN),
    (E1_UP,),
    (E1_DOWN,),
)


def group_of(groups, kind):
    return next(i for i, kinds in enumerate(groups) if kind in kinds)


def cell_state(w):
    density, v0, v1, v2, pressure, b0, b1, b2 = w
    kinetic = 0.5 * density * (v0 * v0 + v1 * v1 + v2 * v2)
    magnetic_sq = b0 * b0 + b1 * b1 + b2 * b2
    energy = pressure / (GAMMA - 1.0) + kinetic + 0.5 * magnetic_sq
    conserved = [density, density * v0, density * v1, density * v2, energy]
    return conserved, magnetic_sq


def flux(w, conserved, magnetic_sq, direction):
    density, v0, v1, v2, pressure, b0, b1, b2 = w
    velocity = (v0, v1, v2)
    magnetic = (b0, b1, b2)
    moving = velocity[direction]
    normal = magnetic[direction]
    total_press = pressure + 0.5 * magnetic_sq
    alignment = v0 * b0 + v1 * b1 + v2 * b2
    fast = jnp.sqrt((GAMMA * pressure + magnetic_sq) / density)
    out = [conserved[direction + 1]]
    for component in range(3):
        moment = conserved[component + 1] * moving - magnetic[component] * normal
        if component == direction:
            moment = moment + total_press
        out.append(moment)
    out.append((conserved[4] + total_press) * moving - normal * alignment)
    return out, jnp.abs(moving) + fast


def quantities(w, direction):
    conserved, magnetic_sq = cell_state(w)
    fluxes, speed = flux(w, conserved, magnetic_sq, direction)
    return conserved, fluxes, speed


def face_flux(lower, upper):
    u_low, f_low, s_low = lower
    u_up, f_up, s_up = upper
    half = 0.5 * jnp.maximum(s_low, s_up)
    return [0.5 * (f_low[i] + f_up[i]) - half * (u_up[i] - u_low[i]) for i in range(5)]


def emf(w, component):
    a, b = ((2, 3), (3, 1), (1, 2))[component]
    return -(w[a] * w[b + 4] - w[b] * w[a + 4])


def kernel(
    cells_hbm, faces_hbm, state, faces_new,
    cv, fv, first_rows, rlo, rhi, f0hi, packs, gp, th_src, gt, f1_src, f1hi, cr_src, cr, pr, e1_corner, e1_src, e1g, e1f, tokens,
    load_sem, send_sem, recv_sem, ok_near, ok_wrap, ok_th,
):
    row = lax.axis_index("row")
    th = lax.axis_index("th")
    ph = lax.axis_index("ph")
    rows, ths, phs = lax.axis_size("row"), lax.axis_size("th"), lax.axis_size("ph")
    z = th * phs + ph
    depth = ths * phs
    at_bottom, at_top = row == 0, row == rows - 1
    at_north, at_south = th == 0, th == ths - 1
    first_z = z == 0
    corner_place = z == 2 * phs - 1
    beside_corner = z == 2 * phs - 2
    corner_sender = (corner_place & (row > 0)) | ((z == phs) & (row == 0))

    def place(dr=0, dt=0, dp=0):
        return {"row": row + dr, "th": th + dt, "ph": lax.rem(ph + dp + phs, phs)}

    load_cells = pltpu.make_async_copy(cells_hbm, cv, load_sem.at[0])
    load_faces = pltpu.make_async_copy(faces_hbm, fv, load_sem.at[0])
    load_velocity = pltpu.make_async_copy(cells_hbm.at[2:4, :, 0:8], first_rows.at[0:2], load_sem.at[1])
    load_field = pltpu.make_async_copy(cells_hbm.at[6:8, :, 0:8], first_rows.at[2:4], load_sem.at[1])

    @pl.when(corner_sender)
    def _():
        load_velocity.start()
        load_field.start()

    load_cells.start()
    load_faces.start()

    barrier = pltpu.get_barrier_semaphore()

    def tell(semaphore, condition, target):
        @pl.when(condition)
        def _():
            pl.semaphore_signal(semaphore, inc=1, device_id=target, device_id_type=MESH)

    def told(semaphore, condition):
        @pl.when(condition)
        def _():
            pl.semaphore_wait(semaphore, 1)

    has_up, has_down = th < ths - 1, th > 0
    first_p, last_p = ph == 0, ph == phs - 1
    inner_up, inner_down = ph < phs - 1, ph > 0
    row_up, row_down = row < rows - 1, row > 0
    plain = jnp.logical_not(corner_place)
    tell(barrier, row_up & plain, place(dr=1))
    tell(barrier, row_down & plain, place(dr=-1))
    tell(barrier, corner_place, place(dp=-1))
    edge = last_p & has_up
    before_edge = first_p & has_down
    twin_below = (th == ths - 2) & inner_up
    twin_above = at_south & inner_up
    past_edge = {"row": row, "th": th + 1, "ph": ph * 0}
    tell(barrier, twin_above, place(dt=-1))
    tell(barrier, edge, past_edge)
    tell(barrier, inner_up, place(dp=1))
    tell(barrier, has_up, place(dt=1))
    tell(barrier, first_p, place(dp=-1))
    tell(barrier, (z == 0) & (row > 0), {"row": row, "th": 1, "ph": phs - 1})
    tell(barrier, (z == 1) & (row == 0), {"row": row, "th": 1, "ph": 0})

    def leaving(kind):
        return (load_sem.at[0], send_sem, load_sem.at[1])[group_of(LEAVE, kind)]

    def copy(kind, src, dst, target, recv=None):
        return pltpu.make_async_remote_copy(
            src_ref=src, dst_ref=dst, send_sem=leaving(kind),
            recv_sem=recv_sem.at[group_of(ARRIVE, kind if recv is None else recv)],
            device_id=target, device_id_type=MESH,
        )

    up_r, down_r = place(dr=1), place(dr=-1)
    up_t, down_t = place(dt=1), place(dt=-1)
    up_p, down_p = place(dp=1), place(dp=-1)
    origin = {"row": row, "th": th * 0, "ph": (row == 0).astype(jnp.int32)}
    copies = {
        ROW_UP: copy(ROW_UP, cv.at[:, 3], rlo, up_r),
        ROW_DOWN: copy(ROW_DOWN, cv.at[:, 0], rhi, down_r),
        FACE_R: copy(FACE_R, fv.at[0, 0], f0hi, down_r),
        PACK_UP: copy(PACK_UP, packs.at[1], gp.at[0], up_p),
        PACK_DOWN: copy(PACK_DOWN, packs.at[0], gp.at[1], down_p),
        TH_UP: copy(TH_UP, th_src.at[1], gt.at[0], up_t),
        TH_DOWN: copy(TH_DOWN, th_src.at[0], gt.at[1], down_t),
        FACE_T: copy(FACE_T, f1_src, f1hi, down_t),
        CORNER_UP: copy(CORNER_UP, cr_src.at[1], cr.at[0], up_t),
        CORNER_DOWN: copy(CORNER_DOWN, cr_src.at[0], cr.at[1], down_t),
        PAIR_UP: copy(PAIR_UP, gp, pr.at[0], up_r),
        PAIR_DOWN: copy(PAIR_DOWN, gp, pr.at[1], down_r),
        E1_UP: copy(E1_UP, e1_src.at[1], e1g.at[0], up_t),
        E1_DOWN: copy(E1_DOWN, e1_src.at[0], e1g.at[1], down_t),
        LOW_UP: copy(LOW_UP, e1g.at[0], e1f.at[0, 0], up_p),
        LOW_DOWN: copy(LOW_DOWN, e1g.at[0], e1f.at[1, 0], down_p),
        HIGH_UP: copy(HIGH_UP, e1g.at[1], e1f.at[0, 1], up_p),
        HIGH_DOWN: copy(HIGH_DOWN, e1g.at[1], e1f.at[1, 1], down_p),
    }
    edge_up = copy(EDGE, e1_src.at[1], e1f.at[0, 0], past_edge, LOW_UP)
    direct_left = copy(DIRECT, e1_corner, e1f.at[0, 1], origin, HIGH_UP)

    def send(kind, condition=None):
        if condition is None:
            copies[kind].start()
        else:
            pl.when(condition)(copies[kind].start)

    def take(semaphore, size, condition=None):
        part = tokens.at[0:size]
        wait = pltpu.make_async_copy(part, part, semaphore).wait
        if condition is None:
            wait()
        else:
            pl.when(condition)(wait)

    def take_sides(semaphore, first, first_size, second, second_size):
        take(semaphore, first_size + second_size, first & second)
        take(semaphore, first_size, first & jnp.logical_not(second))
        take(semaphore, second_size, second & jnp.logical_not(first))

    def arrived(kind):
        return recv_sem.at[group_of(ARRIVE, kind)]

    @pl.when(corner_sender)
    def _():
        pltpu.make_async_copy(first_rows, first_rows, load_sem.at[1]).wait()
        for r in range(4):
            w = [first_rows[k, r, 0:1] for k in range(4)]
            e1_corner[r : r + 1] = -(w[0] * w[3] - w[1] * w[2])

    def number(*conditions):
        total = jnp.int32(0)
        for condition in conditions:
            total = total + condition.astype(jnp.int32)
        return total

    pl.semaphore_wait(
        barrier,
        number(corner_sender, has_down, last_p, row_down & plain, row_up & plain, inner_down, beside_corner)
        + number(before_edge, twin_below),
    )
    pl.when(corner_sender)(direct_left.start)
    tell(ok_th, has_down & jnp.logical_not(twin_above), place(dt=-1))
    tell(ok_wrap, before_edge, {"row": row, "th": th - 1, "ph": ph * 0 + phs - 1})
    tell(ok_wrap, last_p, place(dp=1))
    tell(ok_near, inner_down & plain, place(dp=-1))
    tell(ok_near, beside_corner & row_up, place(dr=1))
    tell(ok_near, beside_corner & row_down, place(dr=-1))

    take(load_sem.at[0], 704)
    send(ROW_UP, row_up & plain)
    send(ROW_DOWN, row_down & plain)
    for r in range(4):
        for f in range(8):
            th_src[0, f * 4 + r : f * 4 + r + 1] = cv[f, r, 0:1]
            th_src[1, f * 4 + r : f * 4 + r + 1] = cv[f, r, 15:16]
    for side in range(2):
        e1_src[side] = emf([th_src[side, f * 4 : f * 4 + 4] for f in range(8)], 0)
    send(E1_DOWN, has_down)
    send(E1_UP, twin_below)
    send(FACE_R, row_down & plain)
    for r in range(4):
        f1_src[r : r + 1] = fv[1, r, 0:1]
    third = fv[2].reshape(64, 128)
    turned = jnp.concatenate([third, third], axis=0).T
    for c in range(4, 8):
        packs[0, c : c + 1] = turned[0:1]
        packs[1, c : c + 1] = turned[127:128]
    send(TH_DOWN, has_down)
    send(FACE_T, has_down)
    send(TH_UP, twin_below)
    for c in range(4):
        turned = cv[2 * c : 2 * c + 2].reshape(128, 128).T
        packs[0, c : c + 1] = turned[0:1]
        packs[1, c : c + 1] = turned[127:128]

    @pl.when(at_bottom)
    def _():
        rlo[...] = cv[:, 0]

    @pl.when(at_top)
    def _():
        rhi[...] = cv[:, 3]
        f0hi[...] = fv[0, 3]

    def fill_polar(side, condition):
        @pl.when(condition)
        def _():
            for f in range(8):
                rows_f = th_src[side, f * 4 : f * 4 + 4]
                gt[side, f * 4 : f * 4 + 4] = -rows_f if f in (2, 7) else rows_f

    fill_polar(0, at_north)
    fill_polar(1, at_south)

    def ghost_rows(side):
        return [gt[side, f * 4 : f * 4 + 4] for f in range(8)]

    @pl.when(at_north)
    def _():
        e1g[0] = emf(ghost_rows(0), 0)

    @pl.when(at_south)
    def _():
        e1g[1] = emf(ghost_rows(1), 0)

    send(PACK_DOWN, inner_down)
    send(PACK_UP, last_p)
    send(LOW_DOWN, at_north & inner_down)
    send(LOW_UP, at_north & last_p)

    @pl.when(beside_corner)
    def _():
        pl.semaphore_wait(ok_near, number(row_up, row_down))

    tell(ok_near, beside_corner, place(dp=1))
    told(ok_near, corner_place)
    send(ROW_UP, row_up & corner_place)
    send(ROW_DOWN, row_down & corner_place)
    send(FACE_R, row_down & corner_place)

    take_sides(arrived(ROW_UP), row_down, 128, row_up, 144)
    for side, line in ((0, 0), (1, 15)):
        for k, ghost in enumerate((rlo, rhi)):
            w = [ghost[f, line : line + 1] for f in range(8)]
            cr_src[side, k : k + 1] = emf(w, 2)

    def fill_corner(side, line, condition):
        @pl.when(condition)
        def _():
            for k, ghost in enumerate((rlo, rhi)):
                w = [ghost[f, line : line + 1] for f in range(8)]
                w[2] = -w[2]
                cr[side, k : k + 1] = emf(w, 2)

    fill_corner(0, 0, at_north)
    fill_corner(1, 15, at_south)
    send(CORNER_DOWN, has_down)
    send(CORNER_UP, twin_below)

    told(ok_near, inner_up & jnp.logical_not(beside_corner))
    send(PACK_UP, inner_up)
    send(LOW_UP, at_north & inner_up)

    shape = (4, 16, 128)
    lane = lax.broadcasted_iota(jnp.int32, shape, 2)
    line = lax.broadcasted_iota(jnp.int32, shape, 1)
    own = [cv[f] for f in range(8)]

    def ahead_t(x):
        return pltpu.roll(x, 15, 1)

    def behind_t(x):
        return pltpu.roll(x, 1, 1)

    def ahead_p(x):
        return pltpu.roll(x, 127, 2)

    def behind_p(x):
        return pltpu.roll(x, 1, 2)

    low = quantities([rlo[f][None] for f in range(8)], 0)
    mid = quantities(own, 0)
    high = quantities([rhi[f][None] for f in range(8)], 0)

    def tall(a, b, c):
        return jnp.concatenate([a, b, c], axis=0)

    u6 = [tall(low[0][i], mid[0][i], high[0][i]) for i in range(5)]
    g6 = [tall(low[1][i], mid[1][i], high[1][i]) for i in range(5)]
    s6 = tall(low[2], mid[2], high[2])
    face = face_flux(([u[:-1] for u in u6], [g[:-1] for g in g6], s6[:-1]), ([u[1:] for u in u6], [g[1:] for g in g6], s6[1:]))
    for i in range(5):
        state[i] = mid[0][i] - STEP * (face[i][1:] - face[i][:-1])

    told(ok_wrap, first_p | edge)
    pl.when(edge)(edge_up.start)
    send(PACK_DOWN, first_p)
    send(LOW_DOWN, at_north & first_p)

    def send_up(condition):
        told(ok_th, condition)
        send(E1_UP, condition)
        send(TH_UP, condition)
        send(CORNER_UP, condition)

    send_up(has_up & last_p)

    take(arrived(PACK_UP), 16)
    send(PAIR_UP, row_up)
    send(PAIR_DOWN, row_down)
    columns = jnp.concatenate([gp[0], gp[1]], axis=0).T

    def column(side, c, half):
        col = columns[half * 64 : half * 64 + 64, side * 8 + c : side * 8 + c + 1]
        return jnp.broadcast_to(col, (64, 128)).reshape(shape)

    left, right = lane == 0, lane == 127
    beside = [
        jnp.where(left, column(0, f // 2, f % 2), jnp.where(right, column(1, f // 2, f % 2), own[f]))
        for f in range(8)
    ]
    upper_third = column(1, 4, 0)
    e1_beside, e2_beside = emf(beside, 0), emf(beside, 1)

    def apply(direction, outer, ahead, behind, is_low, is_high):
        mine = quantities(own, direction)
        edge = quantities(outer, direction)

        def shifted(a, b):
            return jnp.where(is_high, b, ahead(a))

        above = (
            [shifted(mine[0][i], edge[0][i]) for i in range(5)],
            [shifted(mine[1][i], edge[1][i]) for i in range(5)],
            shifted(mine[2], edge[2]),
        )
        upper = face_flux(mine, above)
        lower = face_flux(edge, mine)
        for i in range(5):
            below = jnp.where(is_low, lower[i], behind(upper[i]))
            state[i] = state[i] - STEP * (upper[i] - below)

    apply(2, beside, ahead_p, behind_p, left, right)
    send_up(has_up & inner_up & jnp.logical_not(twin_below))

    high_up = jnp.logical_not(((z == phs - 1) & (row > 0)) | ((z == 0) & (row == 0)))

    def pass_high(condition):
        take(arrived(E1_DOWN), 4, has_up & condition)
        send(HIGH_UP, high_up & condition)
        send(HIGH_DOWN, condition)

    pass_high(last_p)
    take(arrived(E1_UP), 4, has_down)
    send(LOW_UP, has_down & inner_up)
    send(LOW_DOWN, has_down)
    pass_high(inner_up)

    take_sides(arrived(TH_UP), has_down, 34, has_up, 38)

    north, south = line == 0, line == 15

    def spread(ref, *index):
        return jnp.concatenate([jnp.broadcast_to(ref[index + (slice(start, start + 1),)], (16, 128))[None] for start in spread.rows], axis=0)

    def polar(f):
        spread.rows = [f * 4 + r for r in range(4)]
        return jnp.where(north, spread(gt, 0), jnp.where(south, spread(gt, 1), own[f]))

    outside = [polar(f) for f in range(8)]
    apply(1, outside, ahead_t, behind_t, north, south)
    e1_outside, e3_outside = emf(outside, 0), emf(outside, 2)

    take_sides(arrived(PAIR_UP), row_down, 16, row_up, 16)

    def pair_emf(ref, *index):
        rows8 = ref[index] if index else ref[...]
        return -(rows8[1:2] * rows8[2:3] - rows8[0:1] * rows8[3:4])

    pair_rows = [pair_emf(gp, 0), pair_emf(gp, 1), pair_emf(pr, 0, 0), pair_emf(pr, 0, 1), pair_emf(pr, 1, 0), pair_emf(pr, 1, 1)]
    pair_columns = jnp.concatenate(pair_rows + [pair_rows[0], pair_rows[0]], axis=0).T

    def pair_ghost(side):
        lanes = lane[:1]
        parts = []
        for k in range(2):
            near = pair_columns[64:80, k : k + 1] if side == 0 else pair_columns[112:128, k : k + 1]
            far_col = pair_columns[112:128, 2 + k : 3 + k] if side == 0 else pair_columns[64:80, 4 + k : 5 + k]
            edge = at_bottom if side == 0 else at_top
            parts.append(jnp.broadcast_to(jnp.where(edge, near, far_col), (16, 128))[None])
        return jnp.where(lanes == 0, parts[0], parts[1])

    def corner_ghost(k):
        a = jnp.broadcast_to(cr[0, k : k + 1], (16, 128))[None]
        b = jnp.broadcast_to(cr[1, k : k + 1], (16, 128))[None]
        return jnp.where(line[:1] == 0, a, b)

    low_w = [rlo[f][None] for f in range(8)]
    high_w = [rhi[f][None] for f in range(8)]
    e1 = emf(own, 0)
    e2 = tall(emf(low_w, 1), emf(own, 1), emf(high_w, 1))
    e3 = tall(emf(low_w, 2), emf(own, 2), emf(high_w, 2))
    e2_side = tall(pair_ghost(0), e2_beside, pair_ghost(1))
    e3_side = tall(corner_ghost(0), e3_outside, corner_ghost(1))

    six = (6, 16, 128)
    lane6 = lax.broadcasted_iota(jnp.int32, six, 2)
    line6 = lax.broadcasted_iota(jnp.int32, six, 1)
    across_t = jnp.where(line6 == 15, e3_side, ahead_t(e3)) - jnp.where(line6 == 0, e3_side, behind_t(e3))
    across_p = jnp.where(lane6 == 127, e2_side, ahead_p(e2)) - jnp.where(lane6 == 0, e2_side, behind_p(e2))
    curl = across_t - across_p
    new_first = fv[0] - QUARTER * (curl[:4] + curl[1:5])
    new_last = f0hi[...] - QUARTER * (curl[4] + curl[5])
    faces_new[0] = new_first
    last = jnp.where(at_top, new_first[3], new_last)
    state[5] = 0.5 * (new_first + jnp.concatenate([new_first[1:], last[None]], axis=0))

    zero = jnp.zeros(shape, jnp.float32)
    curl = (e2[2:] - e2[:-2]) - (
        jnp.where(south, e1_outside, ahead_t(e1)) - jnp.where(north, e1_outside, behind_t(e1))
    )
    curl_beside = (e2_side[2:] - e2_side[:-2]) - (
        jnp.where(south, zero, ahead_t(e1_beside)) - jnp.where(north, zero, behind_t(e1_beside))
    )
    new_third = fv[2] - QUARTER * (curl + jnp.where(left, curl_beside, behind_p(curl)))
    new_upper = upper_third - QUARTER * (curl + curl_beside)
    faces_new[2] = new_third
    state[7] = 0.5 * (new_third + jnp.where(right, new_upper, ahead_p(new_third)))

    curl = (
        jnp.where(right, e1_beside, ahead_p(e1)) - jnp.where(left, e1_beside, behind_p(e1))
    ) - (e3[2:] - e3[:-2])
    curl_outside = (
        jnp.where(right, zero, ahead_p(e1_outside)) - jnp.where(left, zero, behind_p(e1_outside))
    ) - (e3_side[2:] - e3_side[:-2])
    new_second = fv[1] - QUARTER * (curl + jnp.where(north, curl_outside, behind_t(curl)))
    spread.rows = [0, 1, 2, 3]
    new_upper = spread(f1hi) - QUARTER * (curl + curl_outside)
    new_upper = jnp.where(at_south, 0.0, new_upper)
    faces_new[1] = new_second
    state[6] = 0.5 * (new_second + jnp.where(south, new_upper, ahead_t(new_second)))

    take_sides(leaving(ROW_UP), row_up, 144, row_down, 160)
    take_sides(leaving(TH_UP), has_up, 38, has_down, 42)
    extra = number(inner_up | at_north, high_up, corner_sender, edge)
    for k in range(5):
        take(leaving(PACK_UP), 24 + 4 * k, extra == k)

    lane4 = lax.broadcasted_iota(jnp.int32, (4, 128), 1)

    def from_left(k):
        return QUARTER * jnp.where(lane4 == 0, pltpu.roll(e1f[0, k], 1, 1), 0.0)

    def from_right(k):
        return QUARTER * jnp.where(lane4 == 127, pltpu.roll(e1f[1, k], 127, 1), 0.0)

    keep = jnp.where(at_south, 0.0, 0.5)

    def adjust(ref, r, place_row, amount):
        ref[r, place_row : place_row + 1] = ref[r, place_row : place_row + 1] + amount

    take(arrived(LOW_DOWN), 8)
    b_low, b_high = from_right(0), from_right(1)
    for r in range(4):
        b = b_low[r : r + 1]
        adjust(faces_new.at[1], r, 0, -b)
        adjust(state.at[6], r, 0, -0.5 * b)
        adjust(state.at[7], r, 0, -0.5 * b)
        b = b_high[r : r + 1]
        adjust(state.at[6], r, 15, -keep * b)
        adjust(state.at[7], r, 15, 0.5 * b)
    take(arrived(LOW_UP), 8)
    a_low, a_high = from_left(0), from_left(1)
    for r in range(4):
        a = a_low[r : r + 1]
        adjust(faces_new.at[1], r, 0, a)
        adjust(state.at[6], r, 0, 0.5 * a)
        adjust(faces_new.at[2], r, 0, -a)
        adjust(state.at[7], r, 0, -0.5 * a)
        a = a_high[r : r + 1]
        adjust(state.at[6], r, 15, keep * a)
        adjust(faces_new.at[2], r, 15, a)
        adjust(state.at[7], r, 15, 0.5 * a)


def write_out(state, faces_new, state_hbm, faces_hbm, tokens, sem):
    pltpu.make_async_copy(state, state_hbm, sem).start()
    pltpu.make_async_copy(faces_new, faces_hbm, sem).start()
    pltpu.make_async_copy(tokens, tokens, sem).wait()


def on_device(cells, faces):
    f32 = jnp.float32
    shapes = ((8, 4, 16, 128), (3, 4, 16, 128))
    outputs = pl.pallas_call(
        kernel,
        out_shape=tuple(pltpu.VMEM(shape, f32) for shape in shapes),
        in_specs=[pl.BlockSpec(memory_space=pl.ANY)] * 2,
        out_specs=(pl.BlockSpec(memory_space=pltpu.VMEM),) * 2,
        scratch_shapes=[
            pltpu.VMEM((8, 4, 16, 128), f32),
            pltpu.VMEM((3, 4, 16, 128), f32),
            pltpu.VMEM((4, 4, 8, 128), f32),
            pltpu.VMEM((8, 16, 128), f32),
            pltpu.VMEM((8, 16, 128), f32),
            pltpu.VMEM((16, 128), f32),
            pltpu.VMEM((2, 8, 128), f32),
            pltpu.VMEM((2, 8, 128), f32),
            pltpu.VMEM((2, 32, 128), f32),
            pltpu.VMEM((2, 32, 128), f32),
            pltpu.VMEM((4, 128), f32),
            pltpu.VMEM((4, 128), f32),
            pltpu.VMEM((2, 2, 128), f32),
            pltpu.VMEM((2, 2, 128), f32),
            pltpu.VMEM((2, 2, 8, 128), f32),
            pltpu.VMEM((4, 128), f32),
            pltpu.VMEM((2, 4, 128), f32),
            pltpu.VMEM((2, 4, 128), f32),
            pltpu.VMEM((2, 2, 4, 128), f32),
            pltpu.VMEM((704, 1, 128), f32),
            pltpu.SemaphoreType.DMA((2,)),
            pltpu.SemaphoreType.DMA,
            pltpu.SemaphoreType.DMA((len(ARRIVE),)),
            pltpu.SemaphoreType.REGULAR,
            pltpu.SemaphoreType.REGULAR,
            pltpu.SemaphoreType.REGULAR,
        ],
        name="section",
        compiler_params=pltpu.CompilerParams(collective_id=0, has_side_effects=True),
    )(cells, faces)
    return pl.pallas_call(
        write_out,
        out_shape=tuple(jax.ShapeDtypeStruct(shape, f32) for shape in shapes),
        in_specs=[pl.BlockSpec(memory_space=pltpu.VMEM)] * 2,
        out_specs=(pl.BlockSpec(memory_space=pl.ANY),) * 2,
        scratch_shapes=[pltpu.VMEM((11, 4, 16, 128), f32), pltpu.SemaphoreType.DMA],
        name="write_out",
    )(*(pltpu.with_memory_space_constraint(x, pltpu.VMEM) for x in outputs))


def solution(mesh):
    spec = P(None, "row", "th", "ph")
    return jax.shard_map(on_device, mesh=mesh, in_specs=(spec, spec), out_specs=(spec, spec), check_vma=False)
```
